32 devices in a mesh: fsdp: 32 (over z, y, x, core), dp: 1.
Axes of the slice: x: 2, y: 2, z: 4, core: 2. Of those that a mesh axis runs over, the one named last changes fastest.
Arguments:
- inputs: bfloat16 [8192, 2560], P(('fsdp', 'dp')), may hold values from -6 to 6
- value_cotangent: bfloat16 [8192, 512], P(('fsdp', 'dp')), may hold values from -0.15625 to 0.15625
- master: float32 [2560, 4, 128], P('fsdp', None, 'dp'), may hold values from -0.125 to 0.125
- first_moment: float32 [2560, 4, 128], P('fsdp', None, 'dp'), may hold values from -6 to 6
- second_moment: float32 [2560, 4, 128], P('fsdp', None, 'dp'), may hold values from 0.25 to 4
Outputs:
- moment_one_new: float32 [2560, 4, 128], P('fsdp', None, 'dp')
- moment_two_new: float32 [2560, 4, 128], P('fsdp', None, 'dp')
- master_new: float32 [2560, 4, 128], P('fsdp', None, 'dp')
- head_blocks: bfloat16 [32, 2560, 128], P('fsdp', None, 'dp')
The draws below stay inside these ranges and needn't reach their ends.
All inputs are finite; a program needn't handle non-finite values.
Results may differ from the reference program's by a relative error of at most 0.0018.
Values may be sent and summed in bfloat16 or wider, within the bound.
A program may use at most 64 MiB of HBM per device.

```python
import math
import jax
import jax.numpy as jnp
from jax import lax

D_IN = 2560
KVH = 4
HEAD = 128
STEP = 8
TOK_DEV = 256
VW = 512
TOKENS_ALL = 8192
N_FSDP = 32
N_DP = 1


def strengthened(entries, rng, source, target, parts, factor):
    def block_of(axis_at):
        return (jnp.arange(entries.shape[axis_at]) // (entries.shape[axis_at] // parts)).reshape((-1,) + (1,) * (entries.ndim - 1 - axis_at))

    first = jax.random.permutation(rng, parts)[block_of(target)]
    far = (block_of(target) + parts // 2) % parts
    return jnp.where((block_of(source) == first) | (block_of(source) == far), factor * entries, entries)


def block_levels(stream_key, shape, cuts, smallest, largest):
    gain = 1.0
    for axis_at, blocks in cuts:
        heights = jax.random.uniform(jax.random.fold_in(jax.random.fold_in(stream_key, 6), axis_at), (blocks,), jnp.float32, smallest / len(cuts), largest / len(cuts))
        gain = gain * jnp.repeat(jnp.exp(heights), shape[axis_at] // blocks).reshape((-1,) + (1,) * (len(shape) - 1 - axis_at))
    return gain


def bell_draw(rng, extent, scale, limit, split=(), dtype=jnp.bfloat16):
    array = scale * jax.random.normal(rng, extent, jnp.float32)
    if split:
        array = array * block_levels(rng, extent, split, -0.22, 0.18)
    return jnp.clip(array, -limit, limit).astype(dtype)


def gaussian_with(key, shape, scale, limit, split, heavy, held_as=jnp.bfloat16):
    entries = scale * jax.random.normal(key, shape, jnp.float32)
    if split:
        entries = entries * block_levels(key, shape, split, -0.22, 0.18)
    return jnp.clip(strengthened(entries, jax.random.fold_in(key, 3), *heavy), -limit, limit).astype(held_as)


def setup_inputs(seed: int = 0) -> dict:
    splits = jax.random.split(jax.random.key(seed), 6)
    return {
        "inputs": gaussian_with(splits[0], (TOKENS_ALL, D_IN), 1.0, 6.0, ((0, 32),), (0, 1, 32, 2.75)),
        "value_cotangent": bell_draw(splits[1], (TOKENS_ALL, VW), ((TOK_DEV * N_FSDP * N_DP) ** -0.5), 0.15625, ((0, 32),)),
        "master": bell_draw(splits[2], (D_IN, KVH, HEAD), D_IN ** -0.5, 0.125, ((0, 32),), jnp.float32),
        "first_moment": bell_draw(splits[3], (D_IN, KVH, HEAD), 1.0, 6.0, ((0, 32),), jnp.float32),
        "second_moment": jnp.clip(jnp.exp(math.log(4.0) - 2.7725887 * jax.random.uniform(splits[4], (D_IN, KVH, HEAD), jnp.float32) ** block_levels(splits[4], (D_IN, KVH, HEAD), ((0, 32),), -0.2, 0.2)), 0.25, 4.0),
    }


beta_first = 0.9
beta_second = 0.95
learn_rate = 0.001
weight_decay = 0.1
epsilon = 1e-08

def reference(inputs, value_cotangent, master, first_moment, second_moment):
    gradient = lax.dot_general(inputs, value_cotangent, (((0,), (0,)), ((), ())), preferred_element_type=jnp.float32)
    gradient = gradient.reshape(D_IN, KVH, HEAD)
    moment_one_new = beta_first * first_moment + (1.0 - beta_first) * gradient
    moment_two_new = beta_second * second_moment + (1.0 - beta_second) * gradient * gradient
    correct_one = 1.0 - beta_first ** STEP
    correct_two = 1.0 - beta_second ** STEP
    update = moment_one_new / correct_one / (jnp.sqrt(moment_two_new / correct_two) + epsilon) + weight_decay * master
    master_new = master - learn_rate * update
    narrow_weight = master_new.astype(jnp.bfloat16)
    head_order = (jnp.arange(N_FSDP) % KVH).astype(jnp.int32)
    picked = jnp.take(narrow_weight, head_order, axis=1)
    head_blocks = jnp.transpose(picked, (1, 0, 2))
    return (moment_one_new, moment_two_new, master_new, head_blocks)
```

```python
import functools

import jax
import jax.numpy as jnp
from jax import lax
from jax.experimental import pallas as pl
from jax.experimental.pallas import tpu as pltpu
from jax.sharding import PartitionSpec as P

STEP = 8


beta_first = 0.9
beta_second = 0.95
learn_rate = 0.001
weight_decay = 0.1
epsilon = 1e-08


def adam_update(gradient, moment_one, moment_two, weights):
    moment_one_new = beta_first * moment_one + (1.0 - beta_first) * gradient
    moment_two_new = beta_second * moment_two + (1.0 - beta_second) * gradient * gradient
    correct_one = 1.0 - beta_first**STEP
    correct_two = 1.0 - beta_second**STEP
    update = (
        moment_one_new / correct_one / (jnp.sqrt(moment_two_new / correct_two) + epsilon)
        + weight_decay * weights
    )
    return (moment_one_new, moment_two_new, weights - learn_rate * update)


def shards(inputs, value_cotangent, master, first_moment, second_moment):
    _, heads, slice_width = master.shape
    head_size = value_cotangent.shape[1] // heads
    head_parts = []
    for head in range(heads):
        head_cot = value_cotangent[:, head * head_size : (head + 1) * head_size]
        head_term = lax.dot_general(
            inputs, head_cot, (((0,), (0,)), ((), ())), preferred_element_type=jnp.float32
        )
        head_parts.append(
            lax.psum_scatter(
                head_term.astype(jnp.bfloat16), "dp", scatter_dimension=1, tiled=True
            ).astype(jnp.float32)
        )
    column_part = jnp.stack(head_parts, axis=1)
    grad_share = lax.psum_scatter(column_part, "fsdp", scatter_dimension=0, tiled=True)
    moment_one_new, moment_two_new, master_new = adam_update(
        grad_share, first_moment, second_moment, master
    )
    narrow_weight = master_new.astype(jnp.bfloat16)
    gathered = lax.all_gather(narrow_weight, "fsdp", axis=0, tiled=True)
    head_index = lax.axis_index("fsdp") % heads
    picked = lax.dynamic_slice_in_dim(gathered, head_index, 1, 1)
    tp_block = picked.reshape(1, gathered.shape[0], slice_width)
    return (moment_one_new, moment_two_new, master_new, tp_block)


VMEM_BYTES = 67043328
SPARE_BYTES = 64 * 1024
PLANE = 8


def step_kernel(
    n, pieces, x_hbm, g_hbm, w_hbm, m_hbm, v_hbm, m_out, v_out, w_out, tp_out,
    x_ref, g_ref, w_ref, m_ref, v_ref,
    mate_x, mate_g, total, parts, first_in, relay, second_in,
    column_part, column_in, blocks,
    load_sem, mate_send, mate_recv, first_send, first_recv, second_send, second_recv,
    column_send, column_recv, row_send, row_recv, side_send, side_recv,
):
    me = lax.axis_index("fsdp")
    z = me // PLANE
    q = lax.rem(me, PLANE)
    y = q // 4
    x = lax.rem(q // 2, 2)
    core = lax.rem(q, 2)
    mate = me + 1 - 2 * core
    x_mate = me + 2 - 4 * x
    y_mate = me + 4 - 8 * y
    depth = n // PLANE
    layers = depth // 2
    rows, heads, head_size = w_ref.shape
    half = x_ref.shape[1] // 2
    tile = half // layers
    worker = z // layers
    turn = z + worker * (depth - 1 - 2 * z)

    def layer(side, t):
        return t + side * (depth - 1 - 2 * t)

    loads = [
        pltpu.make_async_copy(source, target, load_sem.at[i])
        for i, (source, target) in enumerate(
            ((g_hbm, g_ref), (x_hbm, x_ref), (w_hbm, w_ref), (m_hbm, m_ref), (v_hbm, v_ref))
        )
    ]
    for load in loads:
        load.start()

    def to(device):
        return dict(device_id={"fsdp": device}, device_id_type=pl.DeviceIdType.MESH)

    barrier = pltpu.get_barrier_semaphore()
    for step in range(depth):
        for slot in range(4):
            other = lax.rem(z + step, depth) * PLANE + y * 4 + slot
            if step:
                pl.semaphore_signal(barrier, inc=1, **to(other))
            else:
                @pl.when(other != me)
                def _():
                    pl.semaphore_signal(barrier, inc=1, **to(other))
    pl.semaphore_signal(barrier, inc=1, **to(y_mate))
    with jax.named_scope("loads"):
        loads[0].wait()
        loads[1].wait()
    with jax.named_scope("barrier"):
        pl.semaphore_wait(barrier, 4 * depth)

    def columns(side, t):
        return pl.ds(pl.multiple_of(layer(side, t) * tile, 128), tile)

    def rows_of_tile(t):
        return slice(t * tile, (t + 1) * tile)

    swap_g = pltpu.make_async_remote_copy(
        g_ref, mate_g, mate_send.at[0], mate_recv.at[0], **to(mate)
    )
    swap_x = [
        pltpu.make_async_remote_copy(
            x_ref.at[:, columns(1 - core, t)],
            mate_x.at[:, rows_of_tile(t)],
            mate_send.at[1], mate_recv.at[1 + t], **to(mate)
        )
        for t in range(layers)
    ]
    swap_g.start()
    for swap in swap_x:
        swap.start()

    def transposed_dot(left, right):
        return lax.dot_general(
            left, right, (((0,), (0,)), ((), ())), preferred_element_type=jnp.float32
        )

    for t in range(layers):
        total[rows_of_tile(t), :] = transposed_dot(x_ref[:, columns(core, t)], g_ref[...])
    with jax.named_scope("swapg"):
        swap_g.wait_recv()

    def finish_tile(t):
        with jax.named_scope(f"swapx{t}"):
            swap_x[t].wait_recv()
        summed = (
            total[rows_of_tile(t), :]
            + transposed_dot(mate_x[:, rows_of_tile(t)], mate_g[...])
        ).astype(jnp.bfloat16)
        for head in range(heads):
            parts[t, head] = summed[:, head * head_size : (head + 1) * head_size].reshape(
                2, 2, 2, rows, head_size
            )

    def first_copy(k, head):
        t, _, start, count = pieces[k]
        span = pl.ds(start, count)
        if goes_x_first(head):
            source, target = parts.at[t, head, :, 1 - x, :, span], x_mate
        else:
            source, target = parts.at[t, head, 1 - y, :, :, span], y_mate
        return pltpu.make_async_remote_copy(
            source, first_in.at[t, head, :, :, span],
            first_send, first_recv.at[k * heads + head], **to(target)
        )

    def second_copy(k, head):
        t, _, start, count = pieces[k]
        span = pl.ds(start, count)
        return pltpu.make_async_remote_copy(
            relay.at[t, head, :, span], second_in.at[t, head, :, span],
            second_send, second_recv.at[k * heads + head],
            **to(y_mate if goes_x_first(head) else x_mate)
        )

    def column_copy(k, head, side):
        t, group, start, count = pieces[k]
        span = pl.ds(start, count)
        return pltpu.make_async_remote_copy(
            column_part.at[t, head, side, span],
            column_in.at[head, z, span],
            column_send,
            column_recv.at[k],
            **to(layer(core, t) * PLANE + 2 * (q // 2) + side),
        )

    def first(k):
        for head in pieces[k][1]:
            first_copy(k, head).start()

    def second(k):
        t, group, start, count = pieces[k]
        span = slice(start, start + count)
        for head in group:
            with jax.named_scope(f"first{k}_{head}"):
                first_copy(k, head).wait_recv()
            if goes_x_first(head):
                own, came = parts[t, head, 1 - y, x, :, span], first_in[t, head, 1 - y, :, span]
            else:
                own, came = parts[t, head, y, 1 - x, :, span], first_in[t, head, 1 - x, :, span]
            relay[t, head, :, span] = (
                own.astype(jnp.float32) + came.astype(jnp.float32)
            ).astype(jnp.bfloat16)
            second_copy(k, head).start()

    def column(k):
        t, group, start, count = pieces[k]
        span = slice(start, start + count)
        for head in group:
            with jax.named_scope(f"second{k}_{head}"):
                second_copy(k, head).wait_recv()
            came = first_in[t, head, y if goes_x_first(head) else x, :, span]
            value = (
                parts[t, head, y, x, :, span].astype(jnp.float32)
                + came.astype(jnp.float32)
                + second_in[t, head, :, span].astype(jnp.float32)
            ).astype(jnp.bfloat16)
            column_part[t, head, :, span] = value
            for side in range(2):
                own = jnp.logical_and(layer(core, t) == z, core == side)

                @pl.when(jnp.logical_not(own))
                def _():
                    column_copy(k, head, side).start()

                @pl.when(own)
                def _():
                    column_in[head, z, span] = value[side]

    def target_of(layer_to, head):
        return layer_to * PLANE + y * 4 + head

    def row_copy(k, layer_to, head):
        _, _, start, count = pieces[k]
        span = pl.ds(start, count)
        return pltpu.make_async_remote_copy(
            blocks.at[head, span], tp_out.at[me, span],
            row_send, row_recv.at[2 * k + worker], **to(target_of(layer_to, head))
        )

    def update(k):
        t, group, start, count = pieces[k]
        span = slice(start, start + count)

        @pl.when(turn == t)
        def _():
            with jax.named_scope(f"column{k}"):
                for sources, here in ((depth - 1, worker == core), (depth, worker != core)):
                    @pl.when(here)
                    def _():
                        came = column_in.at[pl.ds(0, len(group)), pl.ds(0, sources), pl.ds(0, count)]
                        pltpu.make_async_copy(came, came, column_recv.at[k]).wait()
            news = []
            for head in group:
                gradient = column_in[head, 0, span].astype(jnp.float32)
                for source in range(1, depth):
                    gradient = gradient + column_in[head, source, span].astype(jnp.float32)
                m_new, v_new, w_new = adam_update(
                    gradient, m_ref[span, head, :], v_ref[span, head, :], w_ref[span, head, :]
                )
                narrow = w_new.astype(jnp.bfloat16)
                blocks[head, span] = narrow
                for layer_to in range(depth):
                    @pl.when(target_of(layer_to, head) != me)
                    def _():
                        row_copy(k, layer_to, head).start()

                @pl.when(target_of(z, head) == me)
                def _():
                    tp_out[me, span] = narrow
                news.append((head, m_new, v_new, w_new))
            for head, m_new, v_new, w_new in news:
                m_out[span, head, :] = m_new
                v_out[span, head, :] = v_new
                w_out[span, head, :] = w_new

    def side_copy(k, layer_from):
        _, _, start, count = pieces[k]
        block = tp_out.at[pl.ds(layer_from * PLANE + y * 4, 4), pl.ds(start, count)]
        return pltpu.make_async_remote_copy(block, block, side_send, side_recv, **to(y_mate))

    def forward(k):
        t, group, start, count = pieces[k]

        @pl.when(functools.reduce(jnp.logical_or, [lax.rem(q, 4) == head for head in group]))
        def _():
            for group_worker in range(2):
                layer_from = layer(group_worker, t)
                with jax.named_scope(f"row{k}_{group_worker}"):
                    for slabs, here in ((3, layer_from == z), (4, layer_from != z)):
                        @pl.when(here)
                        def _():
                            came = tp_out.at[pl.ds(0, slabs), pl.ds(0, count)]
                            pltpu.make_async_copy(
                                came, came, row_recv.at[2 * k + group_worker]
                            ).wait()
                side_copy(k, layer_from).start()

    per_tile = len(pieces) // layers
    finish_tile(0)
    issued = 0
    for t in range(layers):
        if t:
            finish_tile(t)
        while issued < min(AHEAD, per_tile * (t + 1)):
            first(issued)
            issued += 1
    for load in loads[2:]:
        load.wait()
    for action, k in schedule(len(pieces)):
        if action == "second":
            second(k)
            if issued < len(pieces):
                first(issued)
                issued += 1
        elif action == "column":
            column(k)
        elif action == "update":
            update(k)
        else:
            forward(k)

    with jax.named_scope("sends"):
        swap_g.wait_send()
        pltpu.make_async_copy(mate_x, mate_x, mate_send.at[1]).wait()
        pltpu.make_async_copy(first_in, first_in, first_send).wait()
        pltpu.make_async_copy(relay, relay, second_send).wait()
        sent = column_part.at[0]
        for _ in range(layers - 1):
            pltpu.make_async_copy(sent, sent, column_send).wait()
        for sides, here in ((1, worker == core), (2, worker != core)):
            @pl.when(here)
            def _():
                last = column_part.at[0, :, pl.ds(0, sides)]
                pltpu.make_async_copy(last, last, column_send).wait()
        slabs = tp_out.at[pl.ds(0, depth * heads - 1)]
        pltpu.make_async_copy(slabs, slabs, row_send).wait()
        slabs = tp_out.at[pl.ds(0, depth * 4)]
        pltpu.make_async_copy(slabs, slabs, side_send).wait()
    with jax.named_scope("last"):
        pltpu.make_async_copy(slabs, slabs, side_recv).wait()


AHEAD = 2
X_FIRST = 2


def goes_x_first(head):
    return head < X_FIRST


def row_pieces(layers, heads, rows):
    return tuple(
        (t, (p, p + 2), 0, rows) for t in range(layers) for p in range(heads // 2)
    )


def schedule(count):
    order = [("second", 0)]
    for k in range(count + 3):
        for action, at in (
            ("second", k + 1), ("column", k), ("forward", k - 3), ("update", k - 1)
        ):
            if 0 <= at < count:
                order.append((action, at))
    return order


def finish_kernel(*refs):
    count = (len(refs) - 1) // 2
    copies = [
        pltpu.make_async_copy(refs[i], refs[count + i], refs[-1].at[i])
        for i in range(count)
    ]
    for copy in copies:
        copy.start()
    for copy in copies:
        copy.wait()


def fused(n, inputs, value_cotangent, master, first_moment, second_moment):
    tokens, features = inputs.shape
    width = value_cotangent.shape[1]
    rows, heads, head_size = master.shape
    half = features // 2
    depth = n // PLANE
    layers = depth // 2
    pieces = row_pieces(layers, heads, rows)
    state = jax.ShapeDtypeStruct(master.shape, jnp.float32)
    slabs = jax.ShapeDtypeStruct((n, rows, head_size), jnp.bfloat16)
    block = jax.ShapeDtypeStruct((1, features, head_size), jnp.bfloat16)
    results = 12 * master.size + 2 * block.size + SPARE_BYTES
    vmem = pl.BlockSpec(memory_space=pltpu.VMEM)
    narrow = jnp.bfloat16
    dma = pltpu.SemaphoreType.DMA
    held = pl.pallas_call(
        functools.partial(step_kernel, n, pieces),
        out_shape=tuple(pltpu.VMEM(a.shape, a.dtype) for a in (state, state, state, slabs)),
        in_specs=[pl.BlockSpec(memory_space=pltpu.HBM)] * 5,
        out_specs=[vmem] * 4,
        scratch_shapes=[
            pltpu.VMEM((tokens, features), narrow),
            pltpu.VMEM((tokens, width), narrow),
            pltpu.VMEM(master.shape, jnp.float32),
            pltpu.VMEM(master.shape, jnp.float32),
            pltpu.VMEM(master.shape, jnp.float32),
            pltpu.VMEM((tokens, half), narrow),
            pltpu.VMEM((tokens, width), narrow),
            pltpu.VMEM((half, width), jnp.float32),
            pltpu.VMEM((layers, heads, 2, 2, 2, rows, head_size), narrow),
            pltpu.VMEM((layers, heads, 2, 2, rows, head_size), narrow),
            pltpu.VMEM((layers, heads, 2, rows, head_size), narrow),
            pltpu.VMEM((layers, heads, 2, rows, head_size), narrow),
            pltpu.VMEM((layers, heads, 2, rows, head_size), narrow),
            pltpu.VMEM((heads, depth, rows, head_size), narrow),
            pltpu.VMEM((heads, rows, head_size), narrow),
            dma((5,)),
            dma((2,)),
            dma((1 + layers,)),
            dma,
            dma((len(pieces) * heads,)),
            dma,
            dma((len(pieces) * heads,)),
            dma,
            dma((len(pieces),)),
            dma,
            dma((2 * len(pieces),)),
            dma,
            dma,
        ],
        compiler_params=pltpu.CompilerParams(
            collective_id=0, has_side_effects=True, vmem_limit_bytes=VMEM_BYTES - results
        ),
    )(inputs, value_cotangent, master, first_moment, second_moment)
    held = held[:3] + (held[3].reshape(block.shape),)
    return pl.pallas_call(
        finish_kernel,
        out_shape=(state, state, state, block),
        in_specs=[vmem] * 4,
        out_specs=[pl.BlockSpec(memory_space=pltpu.HBM)] * 4,
        scratch_shapes=[dma((4,))],
        compiler_params=pltpu.CompilerParams(vmem_limit_bytes=VMEM_BYTES // 2),
    )(*held)


def solution(mesh):
    n = mesh.shape["fsdp"]

    def body(inputs, value_cotangent, master, first_moment, second_moment):
        rows = master.shape[0]
        direct = (
            mesh.shape["dp"] == 1
            and n % (2 * PLANE) == 0
            and inputs.shape[1] % (256 * (n // (2 * PLANE))) == 0
            and rows % 16 == 0
            and master.shape[1] * 2 == PLANE
            and master.shape[2] % 128 == 0
        )
        if direct:
            return fused(n, inputs, value_cotangent, master, first_moment, second_moment)
        return shards(inputs, value_cotangent, master, first_moment, second_moment)

    placed = (
        P(("fsdp", "dp"), None),
        P(("fsdp", "dp"), None),
        P("fsdp", None, "dp"),
        P("fsdp", None, "dp"),
        P("fsdp", None, "dp"),
    )
    return jax.shard_map(
        body,
        mesh=mesh,
        in_specs=placed,
        out_specs=(
            P("fsdp", None, "dp"),
            P("fsdp", None, "dp"),
            P("fsdp", None, "dp"),
            P("fsdp", None, "dp"),
        ),
        check_vma=False,
    )
```

```python
import functools

import jax
import jax.numpy as jnp
from jax import lax
from jax.experimental import pallas as pl
from jax.experimental.pallas import tpu as pltpu
from jax.sharding import PartitionSpec as P

STEP = 8


beta_first = 0.9
beta_second = 0.95
learn_rate = 0.001
weight_decay = 0.1
epsilon = 1e-08


def adam_update(gradient, moment_one, moment_two, weights):
    moment_one_new = beta_first * moment_one + (1.0 - beta_first) * gradient
    moment_two_new = beta_second * moment_two + (1.0 - beta_second) * gradient * gradient
    correct_one = 1.0 - beta_first**STEP
    correct_two = 1.0 - beta_second**STEP
    update = (
        moment_one_new / correct_one / (jnp.sqrt(moment_two_new / correct_two) + epsilon)
        + weight_decay * weights
    )
    return (moment_one_new, moment_two_new, weights - learn_rate * update)


def shards(inputs, value_cotangent, master, first_moment, second_moment):
    _, heads, slice_width = master.shape
    head_size = value_cotangent.shape[1] // heads
    head_parts = []
    for head in range(heads):
        head_cot = value_cotangent[:, head * head_size : (head + 1) * head_size]
        head_term = lax.dot_general(
            inputs, head_cot, (((0,), (0,)), ((), ())), preferred_element_type=jnp.float32
        )
        head_parts.append(
            lax.psum_scatter(
                head_term.astype(jnp.bfloat16), "dp", scatter_dimension=1, tiled=True
            ).astype(jnp.float32)
        )
    column_part = jnp.stack(head_parts, axis=1)
    grad_share = lax.psum_scatter(column_part, "fsdp", scatter_dimension=0, tiled=True)
    moment_one_new, moment_two_new, master_new = adam_update(
        grad_share, first_moment, second_moment, master
    )
    narrow_weight = master_new.astype(jnp.bfloat16)
    gathered = lax.all_gather(narrow_weight, "fsdp", axis=0, tiled=True)
    head_index = lax.axis_index("fsdp") % heads
    picked = lax.dynamic_slice_in_dim(gathered, head_index, 1, 1)
    tp_block = picked.reshape(1, gathered.shape[0], slice_width)
    return (moment_one_new, moment_two_new, master_new, tp_block)


VMEM_BYTES = 67043328
SPARE_BYTES = 64 * 1024
PLANE = 8


def step_kernel(
    n, pieces, x_hbm, g_hbm, w_hbm, m_hbm, v_hbm, m_out, v_out, w_out, tp_out,
    x_ref, g_ref, w_ref, m_ref, v_ref,
    total, mate_part, mate_in, parts, first_in, relay, second_in,
    column_part, column_in, blocks,
    load_sem, mate_send, mate_recv, plane_send, first_recv, second_recv,
    column_send, column_recv, row_send, row_recv, far_send, side_send, side_recv,
    up_sem, down_sem,
):
    me = lax.axis_index("fsdp")
    z = me // PLANE
    q = lax.rem(me, PLANE)
    y = q // 4
    x = lax.rem(q // 2, 2)
    core = lax.rem(q, 2)
    mate = me + 1 - 2 * core
    x_mate = me + 2 - 4 * x
    y_mate = me + 4 - 8 * y
    xy_mate = x_mate + 4 - 8 * y
    depth = n // PLANE
    layers = depth // 2
    rows, heads, head_size = w_ref.shape
    half = x_ref.shape[1] // 2
    tile = half // layers
    worker = z // layers

    def mirrored(place):
        return place + worker * (depth - 1 - 2 * place)

    inward = mirrored(z)

    def layer(side, t):
        return t + side * (depth - 1 - 2 * t)

    loads = [
        pltpu.make_async_copy(source, target, load_sem.at[i])
        for i, (source, target) in enumerate(
            ((g_hbm, g_ref), (x_hbm, x_ref), (w_hbm, w_ref), (m_hbm, m_ref), (v_hbm, v_ref))
        )
    ]
    for load in loads:
        load.start()

    def to(device):
        return dict(device_id={"fsdp": device}, device_id_type=pl.DeviceIdType.MESH)

    barrier = pltpu.get_barrier_semaphore()
    for slot in range(4):
        @pl.when(lax.rem(q, 4) != slot)
        def _():
            pl.semaphore_signal(barrier, inc=1, **to(z * PLANE + y * 4 + slot))
    pl.semaphore_signal(barrier, inc=1, **to(y_mate))
    has_lower, has_upper = z > 0, z < depth - 1

    @pl.when(has_lower)
    def _():
        pl.semaphore_signal(barrier, inc=1, **to(me - PLANE))

    @pl.when(has_upper)
    def _():
        pl.semaphore_signal(barrier, inc=1, **to(me + PLANE))

    def point(p):
        for rank, behind, ahead, semaphore, step in (
            (z, has_lower, has_upper, up_sem, PLANE),
            (depth - 1 - z, has_upper, has_lower, down_sem, -PLANE),
        ):
            @pl.when(rank == p if p < POINTS else rank >= p)
            def _():
                @pl.when(behind)
                def _():
                    pl.semaphore_wait(semaphore, 1)

                @pl.when(ahead)
                def _():
                    pl.semaphore_signal(semaphore, inc=1, **to(me + step))

    with jax.named_scope("loads"):
        loads[0].wait()
        loads[1].wait()

    def dot_tile(side, t):
        columns = pl.ds(pl.multiple_of(layer(side, t) * tile, 128), tile)
        return lax.dot_general(
            x_ref[:, columns], g_ref[...], (((0,), (0,)), ((), ())),
            preferred_element_type=jnp.float32,
        ).reshape(2, 2, 2, rows, heads * head_size)

    def span_of(k):
        start, count = pieces[k][:2]
        return pl.ds(start, count)

    def slice_of(k):
        start, count = pieces[k][:2]
        return slice(start, start + count)

    def mate_copy(k, t):
        span = span_of(k)
        return pltpu.make_async_remote_copy(
            mate_part.at[t, :, :, :, span], mate_in.at[t, :, :, :, span],
            mate_send, mate_recv.at[k * layers + t], **to(mate)
        )

    def first_copies(k, t):
        span = span_of(k)
        arrived = first_recv.at[k * layers + t]
        if not pieces[k][2]:
            moves = (
                (parts.at[t, y, 1 - x, :, span], first_in.at[t, 0, :, span], x_mate),
                (parts.at[t, 1 - y, x, :, span], first_in.at[t, 1, :, span], y_mate),
                (parts.at[t, 1 - y, 1 - x, :, span], second_in.at[t, :, span], xy_mate),
            )
        elif t % 2 == 0:
            moves = ((parts.at[t, :, 1 - x, :, span], first_in.at[t, :, :, span], x_mate),)
        else:
            moves = ((parts.at[t, 1 - y, :, :, span], first_in.at[t, :, :, span], y_mate),)
        return [
            pltpu.make_async_remote_copy(source, target, plane_send, arrived, **to(device))
            for source, target, device in moves
        ]

    def second_copy(k, t):
        span = span_of(k)
        return pltpu.make_async_remote_copy(
            relay.at[t, :, span], second_in.at[t, :, span],
            plane_send, second_recv.at[k * layers + t],
            **to(y_mate if t % 2 == 0 else x_mate)
        )

    def column_copy(k, t, side):
        span = span_of(k)
        return pltpu.make_async_remote_copy(
            column_part.at[t, side, span], column_in.at[z, span],
            column_send, column_recv.at[k],
            **to(layer(core, t) * PLANE + 2 * (q // 2) + side),
        )

    def drain(block, semaphore):
        pltpu.make_async_copy(block, block, semaphore).wait()

    def join(k, t):
        span = slice_of(k)
        with jax.named_scope(f"mate{k}_{t}"):
            mate_copy(k, t).wait_recv()
        parts[t, :, :, :, span] = (
            total[t, :, :, :, span] + mate_in[t, :, :, :, span].astype(jnp.float32)
        ).astype(jnp.bfloat16)
        for copy in first_copies(k, t):
            copy.start()

    def second(k):
        span = slice_of(k)
        if not pieces[k][2]:
            return
        for t in range(layers):
            with jax.named_scope(f"first{k}_{t}"):
                drain(first_in.at[t, :, :, span_of(k)], first_recv.at[k * layers + t])
            if t % 2 == 0:
                own, came = parts[t, 1 - y, x, :, span], first_in[t, 1 - y, :, span]
            else:
                own, came = parts[t, y, 1 - x, :, span], first_in[t, 1 - x, :, span]
            relay[t, :, span] = (
                own.astype(jnp.float32) + came.astype(jnp.float32)
            ).astype(jnp.bfloat16)
            second_copy(k, t).start()

    def column(k):
        span = slice_of(k)
        for t in range(layers):
            if pieces[k][2]:
                with jax.named_scope(f"second{k}_{t}"):
                    second_copy(k, t).wait_recv()
                came = first_in[t, y if t % 2 == 0 else x, :, span].astype(jnp.float32)
            else:
                with jax.named_scope(f"plane{k}_{t}"):
                    for _ in range(3):
                        drain(relay.at[t, :, span_of(k)], first_recv.at[k * layers + t])
                came = first_in[t, 0, :, span].astype(jnp.float32) + first_in[
                    t, 1, :, span
                ].astype(jnp.float32)
            value = (
                parts[t, y, x, :, span].astype(jnp.float32)
                + came
                + second_in[t, :, span].astype(jnp.float32)
            ).astype(jnp.bfloat16)
            column_part[t, :, span] = value
            for side in range(2):
                own = jnp.logical_and(layer(core, t) == z, core == side)

                @pl.when(jnp.logical_not(own))
                def _():
                    column_copy(k, t, side).start()

                @pl.when(own)
                def _():
                    column_in[z, span] = value[side]

    def target_of(layer_to, head):
        return layer_to * PLANE + y * 4 + head

    def reach(k):
        return layers + 1 if pieces[k][3] else depth

    def row_copy(k, layer_to, head):
        span = span_of(k)
        return pltpu.make_async_remote_copy(
            blocks.at[head, span], tp_out.at[me, span],
            row_send, row_recv.at[k * depth + z], **to(target_of(layer_to, head))
        )

    def update(k):
        span = slice_of(k)
        with jax.named_scope(f"column{k}"):
            for sources, here in ((depth - 1, worker == core), (depth, worker != core)):
                @pl.when(here)
                def _():
                    drain(column_in.at[pl.ds(0, sources), span_of(k)], column_recv.at[k])
        gradients = column_in[0, span].astype(jnp.float32)
        for source in range(1, depth):
            gradients = gradients + column_in[source, span].astype(jnp.float32)
        news = []
        for head in range(heads):
            m_new, v_new, w_new = adam_update(
                gradients[:, head * head_size : (head + 1) * head_size],
                m_ref[span, head, :], v_ref[span, head, :], w_ref[span, head, :],
            )
            narrow = w_new.astype(jnp.bfloat16)
            blocks[head, span] = narrow
            news.append((m_new, v_new, w_new))
        for place in reversed(range(reach(k))):
            for head in range(heads):
                target = target_of(mirrored(place), head)

                @pl.when(target != me)
                def _():
                    row_copy(k, mirrored(place), head).start()

        tp_out[me, span] = blocks[lax.rem(q, 4), span]
        for head, (m_new, v_new, w_new) in enumerate(news):
            m_out[span, head, :] = m_new
            v_out[span, head, :] = v_new
            w_out[span, head, :] = w_new

    def group_copy(k, layer_from, device, send, recv):
        block = tp_out.at[pl.ds(layer_from * PLANE + y * 4, 4), span_of(k)]
        return pltpu.make_async_remote_copy(block, block, send, recv, **to(device))

    def forward(k, places, relayed):
        for place in places:
            layer_from = mirrored(place)
            arrived = row_recv.at[k * depth + layer_from]
            with jax.named_scope(f"row{k}_{place}"):
                if place < layers:
                    for slabs, here in ((3, inward == place), (4, inward != place)):
                        @pl.when(here)
                        def _():
                            drain(tp_out.at[pl.ds(0, slabs), span_of(k)], arrived)
                else:
                    drain(tp_out.at[pl.ds(0, 4), span_of(k)], arrived)
            if relayed:
                for other in range(layers - 1):
                    group_copy(
                        k, layer_from, mirrored(other) * PLANE + q, far_send, arrived
                    ).start()
            group_copy(k, layer_from, y_mate, side_send, side_recv).start()

    def near(k):
        forward(k, range(layers), False)

    def gate(k):
        @pl.when(inward == layers - 1)
        def _():
            forward(k, range(layers, depth), pieces[k][3])

    def end(k):
        @pl.when(inward != layers - 1)
        def _():
            forward(k, range(layers, depth), False)

    for t in range(layers):
        mate_part[t] = dot_tile(1 - core, t).astype(jnp.bfloat16)
        if t == 0:
            with jax.named_scope("barrier"):
                pl.semaphore_wait(
                    barrier, 4 + has_lower.astype(jnp.int32) + has_upper.astype(jnp.int32)
                )
            point(0)
        mate_copy(0, t).start()
        total[t] = dot_tile(core, t)
        if t:
            for k in range(1, len(pieces)):
                for other in range(layers):
                    mate_copy(k, other).start()

    for load in loads[2:]:
        load.wait()
    for action, k in ORDER:
        if action == "join":
            for t in range(layers):
                join(k, t)
        elif action == "point":
            with jax.named_scope(f"point{k}"):
                point(k)
        elif action == "second":
            second(k)
        elif action == "column":
            column(k)
        elif action == "update":
            update(k)
        else:
            {"near": near, "gate": gate, "end": end}[action](k)

    with jax.named_scope("sends"):
        drain(mate_part, mate_send)
        for k in range(len(pieces)):
            span = span_of(k)
            if pieces[k][2]:
                drain(first_in.at[:, :, :, span], plane_send)
                drain(relay.at[:, :, span], plane_send)
            else:
                for _ in range(3):
                    drain(relay.at[:, :, span], plane_send)
        for sides, here in ((1, worker == core), (2, worker != core)):
            @pl.when(here)
            def _():
                for t in range(layers):
                    drain(column_part.at[t, pl.ds(0, sides if t == 0 else 2)], column_send)
        for k in range(len(pieces)):
            drain(tp_out.at[pl.ds(0, heads * reach(k) - 1), span_of(k)], row_send)
            if pieces[k][3] and layers > 1:
                @pl.when(inward == layers - 1)
                def _():
                    for _ in range(layers - 1):
                        drain(tp_out.at[pl.ds(0, 4 * layers), span_of(k)], far_send)
        slabs = tp_out.at[pl.ds(0, depth * 4)]
        drain(slabs, side_send)
    with jax.named_scope("last"):
        drain(slabs, side_recv)


POINTS = 3
PARTS = ((16, True, True),) * 5
ORDER = (
    ("join", 0), ("join", 1), ("join", 2), ("point", 1), ("second", 0), ("join", 3),
    ("point", 2), ("second", 1), ("join", 4), ("second", 2), ("point", 3), ("column", 0),
    ("second", 3), ("column", 1), ("second", 4), ("column", 2), ("update", 0), ("column", 3),
    ("column", 4), ("update", 1), ("near", 0), ("gate", 0), ("update", 2), ("near", 1),
    ("update", 3), ("gate", 1), ("end", 0), ("update", 4), ("near", 2), ("gate", 2),
    ("near", 3), ("gate", 3), ("end", 1), ("end", 2), ("near", 4), ("gate", 4), ("end", 3),
    ("end", 4),
)


def row_pieces(rows):
    pieces, start = [], 0
    for i, (share, twice, deputed) in enumerate(PARTS):
        count = rows - start if i + 1 == len(PARTS) else share
        pieces.append((start, count, twice, deputed))
        start += count
    return tuple(pieces)


def finish_kernel(*refs):
    count = (len(refs) - 1) // 2
    copies = [
        pltpu.make_async_copy(refs[i], refs[count + i], refs[-1].at[i])
        for i in range(count)
    ]
    for copy in copies:
        copy.start()
    for copy in copies:
        copy.wait()


def fused(n, inputs, value_cotangent, master, first_moment, second_moment):
    tokens, features = inputs.shape
    width = value_cotangent.shape[1]
    rows, heads, head_size = master.shape
    depth = n // PLANE
    layers = depth // 2
    pieces = row_pieces(rows)
    state = jax.ShapeDtypeStruct(master.shape, jnp.float32)
    slabs = jax.ShapeDtypeStruct((n, rows, head_size), jnp.bfloat16)
    block = jax.ShapeDtypeStruct((1, features, head_size), jnp.bfloat16)
    results = 12 * master.size + 2 * block.size + SPARE_BYTES
    vmem = pl.BlockSpec(memory_space=pltpu.VMEM)
    narrow = jnp.bfloat16
    dma = pltpu.SemaphoreType.DMA
    held = pl.pallas_call(
        functools.partial(step_kernel, n, pieces),
        out_shape=tuple(pltpu.VMEM(a.shape, a.dtype) for a in (state, state, state, slabs)),
        in_specs=[pl.BlockSpec(memory_space=pltpu.HBM)] * 5,
        out_specs=[vmem] * 4,
        scratch_shapes=[
            pltpu.VMEM((tokens, features), narrow),
            pltpu.VMEM((tokens, width), narrow),
            pltpu.VMEM(master.shape, jnp.float32),
            pltpu.VMEM(master.shape, jnp.float32),
            pltpu.VMEM(master.shape, jnp.float32),
            pltpu.VMEM((layers, 2, 2, 2, rows, width), jnp.float32),
            pltpu.VMEM((layers, 2, 2, 2, rows, width), narrow),
            pltpu.VMEM((layers, 2, 2, 2, rows, width), narrow),
            pltpu.VMEM((layers, 2, 2, 2, rows, width), narrow),
            pltpu.VMEM((layers, 2, 2, rows, width), narrow),
            pltpu.VMEM((layers, 2, rows, width), narrow),
            pltpu.VMEM((layers, 2, rows, width), narrow),
            pltpu.VMEM((layers, 2, rows, width), narrow),
            pltpu.VMEM((depth, rows, width), narrow),
            pltpu.VMEM((heads, rows, head_size), narrow),
            dma((5,)),
            dma,
            dma((layers * len(pieces),)),
            dma,
            dma((layers * len(pieces),)),
            dma((layers * len(pieces),)),
            dma,
            dma((len(pieces),)),
            dma,
            dma((depth * len(pieces),)),
            dma,
            dma,
            dma,
            pltpu.SemaphoreType.REGULAR,
            pltpu.SemaphoreType.REGULAR,
        ],
        compiler_params=pltpu.CompilerParams(
            collective_id=0, has_side_effects=True, vmem_limit_bytes=VMEM_BYTES - results
        ),
    )(inputs, value_cotangent, master, first_moment, second_moment)
    held = held[:3] + (held[3].reshape(block.shape),)
    return pl.pallas_call(
        finish_kernel,
        out_shape=(state, state, state, block),
        in_specs=[vmem] * 4,
        out_specs=[pl.BlockSpec(memory_space=pltpu.HBM)] * 4,
        scratch_shapes=[dma((4,))],
        compiler_params=pltpu.CompilerParams(vmem_limit_bytes=VMEM_BYTES // 2),
    )(*held)


def solution(mesh):
    n = mesh.shape["fsdp"]

    def body(inputs, value_cotangent, master, first_moment, second_moment):
        rows = master.shape[0]
        direct = (
            mesh.shape["dp"] == 1
            and n % (2 * PLANE) == 0
            and inputs.shape[1] % (256 * (n // (2 * PLANE))) == 0
            and rows % 16 == 0
            and rows > sum(part[0] for part in PARTS[:-1])
            and master.shape[1] * 2 == PLANE
            and master.shape[2] % 128 == 0
        )
        if direct:
            return fused(n, inputs, value_cotangent, master, first_moment, second_moment)
        return shards(inputs, value_cotangent, master, first_moment, second_moment)

    placed = (
        P(("fsdp", "dp"), None),
        P(("fsdp", "dp"), None),
        P("fsdp", None, "dp"),
        P("fsdp", None, "dp"),
        P("fsdp", None, "dp"),
    )
    return jax.shard_map(
        body,
        mesh=mesh,
        in_specs=placed,
        out_specs=(
            P("fsdp", None, "dp"),
            P("fsdp", None, "dp"),
            P("fsdp", None, "dp"),
            P("fsdp", None, "dp"),
        ),
        check_vma=False,
    )
```

```python
import functools

import jax
import jax.numpy as jnp
from jax import lax
from jax.experimental import pallas as pl
from jax.experimental.pallas import tpu as pltpu
from jax.sharding import PartitionSpec as P

STEP = 8


beta_first = 0.9
beta_second = 0.95
learn_rate = 0.001
weight_decay = 0.1
epsilon = 1e-08


def adam_update(gradient, moment_one, moment_two, weights):
    moment_one_new = beta_first * moment_one + (1.0 - beta_first) * gradient
    moment_two_new = beta_second * moment_two + (1.0 - beta_second) * gradient * gradient
    correct_one = 1.0 - beta_first**STEP
    correct_two = 1.0 - beta_second**STEP
    update = (
        moment_one_new / correct_one / (jnp.sqrt(moment_two_new / correct_two) + epsilon)
        + weight_decay * weights
    )
    return (moment_one_new, moment_two_new, weights - learn_rate * update)


def shards(inputs, value_cotangent, master, first_moment, second_moment):
    _, heads, slice_width = master.shape
    head_size = value_cotangent.shape[1] // heads
    head_parts = []
    for head in range(heads):
        head_cot = value_cotangent[:, head * head_size : (head + 1) * head_size]
        head_term = lax.dot_general(
            inputs, head_cot, (((0,), (0,)), ((), ())), preferred_element_type=jnp.float32
        )
        head_parts.append(
            lax.psum_scatter(
                head_term.astype(jnp.bfloat16), "dp", scatter_dimension=1, tiled=True
            ).astype(jnp.float32)
        )
    column_part = jnp.stack(head_parts, axis=1)
    grad_share = lax.psum_scatter(column_part, "fsdp", scatter_dimension=0, tiled=True)
    moment_one_new, moment_two_new, master_new = adam_update(
        grad_share, first_moment, second_moment, master
    )
    narrow_weight = master_new.astype(jnp.bfloat16)
    gathered = lax.all_gather(narrow_weight, "fsdp", axis=0, tiled=True)
    head_index = lax.axis_index("fsdp") % heads
    picked = lax.dynamic_slice_in_dim(gathered, head_index, 1, 1)
    tp_block = picked.reshape(1, gathered.shape[0], slice_width)
    return (moment_one_new, moment_two_new, master_new, tp_block)


VMEM_BYTES = 67043328
SPARE_BYTES = 64 * 1024
PLANE = 8


def step_kernel(
    n, pieces, x_hbm, g_hbm, w_hbm, m_hbm, v_hbm, m_out, v_out, w_out, tp_out,
    x_ref, g_ref, w_ref, m_ref, v_ref,
    total, mate_part, mate_in, parts, first_in, relay, second_in,
    column_part, column_in, line_in, line_sum, plane_part, plane_in, blocks,
    load_sem, mate_send, mate_recv, plane_send, first_recv, second_recv,
    column_send, column_recv, row_send, row_recv, far_send, side_send, side_recv,
    line_recv, plane_recv, up_sem, down_sem,
):
    me = lax.axis_index("fsdp")
    z = me // PLANE
    q = lax.rem(me, PLANE)
    y = q // 4
    x = lax.rem(q // 2, 2)
    core = lax.rem(q, 2)
    mate = me + 1 - 2 * core
    x_mate = me + 2 - 4 * x
    y_mate = me + 4 - 8 * y
    xy_mate = x_mate + 4 - 8 * y
    depth = n // PLANE
    layers = depth // 2
    rows, heads, head_size = w_ref.shape
    half = x_ref.shape[1] // 2
    tile = half // layers
    worker = z // layers

    def mirrored(place):
        return place + worker * (depth - 1 - 2 * place)

    inward = mirrored(z)

    def layer(side, t):
        return t + side * (depth - 1 - 2 * t)

    loads = [
        pltpu.make_async_copy(source, target, load_sem.at[i])
        for i, (source, target) in enumerate(
            ((g_hbm, g_ref), (x_hbm, x_ref), (w_hbm, w_ref), (m_hbm, m_ref), (v_hbm, v_ref))
        )
    ]
    for load in loads:
        load.start()

    def to(device):
        return dict(device_id={"fsdp": device}, device_id_type=pl.DeviceIdType.MESH)

    barrier = pltpu.get_barrier_semaphore()
    for slot in range(4):
        @pl.when(lax.rem(q, 4) != slot)
        def _():
            pl.semaphore_signal(barrier, inc=1, **to(z * PLANE + y * 4 + slot))
    pl.semaphore_signal(barrier, inc=1, **to(y_mate))
    has_lower, has_upper = z > 0, z < depth - 1

    @pl.when(has_lower)
    def _():
        pl.semaphore_signal(barrier, inc=1, **to(me - PLANE))

    @pl.when(has_upper)
    def _():
        pl.semaphore_signal(barrier, inc=1, **to(me + PLANE))

    def point(p):
        for rank, behind, ahead, semaphore, step in (
            (z, has_lower, has_upper, up_sem, PLANE),
            (depth - 1 - z, has_upper, has_lower, down_sem, -PLANE),
        ):
            @pl.when(rank == p if p < POINTS else rank >= p)
            def _():
                @pl.when(behind)
                def _():
                    pl.semaphore_wait(semaphore, 1)

                @pl.when(ahead)
                def _():
                    pl.semaphore_signal(semaphore, inc=1, **to(me + step))

    with jax.named_scope("loads"):
        loads[0].wait()
        loads[1].wait()

    def dot_tile(side, t):
        columns = pl.ds(pl.multiple_of(layer(side, t) * tile, 128), tile)
        return lax.dot_general(
            x_ref[:, columns], g_ref[...], (((0,), (0,)), ((), ())),
            preferred_element_type=jnp.float32,
        ).reshape(2, 2, 2, rows, heads * head_size)

    def span_of(k):
        start, count = pieces[k][:2]
        return pl.ds(start, count)

    def slice_of(k):
        start, count = pieces[k][:2]
        return slice(start, start + count)

    def mate_copy(k, t):
        span = span_of(k)
        return pltpu.make_async_remote_copy(
            mate_part.at[t, :, :, :, span], mate_in.at[t, :, :, :, span],
            mate_send, mate_recv.at[k * layers + t], **to(mate)
        )

    def first_copies(k, t):
        span = span_of(k)
        arrived = first_recv.at[k * layers + t]
        if t % 2 == 0:
            moves = ((parts.at[t, :, 1 - x, :, span], first_in.at[t, :, :, span], x_mate),)
        else:
            moves = ((parts.at[t, 1 - y, :, :, span], first_in.at[t, :, :, span], y_mate),)
        return [
            pltpu.make_async_remote_copy(source, target, plane_send, arrived, **to(device))
            for source, target, device in moves
        ]

    def second_copy(k, t):
        span = span_of(k)
        return pltpu.make_async_remote_copy(
            relay.at[t, :, span], second_in.at[t, :, span],
            plane_send, second_recv.at[k * layers + t],
            **to(y_mate if t % 2 == 0 else x_mate)
        )

    def column_copy(k, t, side):
        span = span_of(k)
        return pltpu.make_async_remote_copy(
            column_part.at[t, side, span], column_in.at[z, span],
            column_send, column_recv.at[k],
            **to(layer(core, t) * PLANE + 2 * (q // 2) + side),
        )

    def drain(block, semaphore):
        pltpu.make_async_copy(block, block, semaphore).wait()

    def join(k, t):
        span = slice_of(k)
        with jax.named_scope(f"mate{k}_{t}"):
            mate_copy(k, t).wait_recv()
        value = (
            total[t, :, :, :, span] + mate_in[t, :, :, :, span].astype(jnp.float32)
        ).astype(jnp.bfloat16)
        parts[t, :, :, :, span] = value
        if pieces[k][2]:
            for copy in first_copies(k, t):
                copy.start()
            return
        for side in range(2):
            own = jnp.logical_and(layer(core, t) == z, core == side)

            @pl.when(jnp.logical_not(own))
            def _():
                pltpu.make_async_remote_copy(
                    parts.at[t, :, :, side, span_of(k)], line_in.at[z], plane_send, line_recv,
                    **to(layer(core, t) * PLANE + 2 * (q // 2) + side)
                ).start()

            @pl.when(own)
            def _():
                line_in[z] = value[:, :, side]

    def across(k):
        with jax.named_scope(f"line{k}"):
            for sources, here in ((depth - 1, worker == core), (depth, worker != core)):
                @pl.when(here)
                def _():
                    drain(line_in.at[pl.ds(0, sources)], line_recv)
        value = line_in[0].astype(jnp.float32)
        for source in range(1, depth):
            value = value + line_in[source].astype(jnp.float32)
        plane_part[...] = value.astype(jnp.bfloat16)
        for slot, (row, column_at, device) in enumerate(
            ((y, 1 - x, x_mate), (1 - y, x, y_mate), (1 - y, 1 - x, xy_mate))
        ):
            pltpu.make_async_remote_copy(
                plane_part.at[row, column_at], plane_in.at[slot], plane_send, plane_recv,
                **to(device)
            ).start()
        own = line_in[0, y, x].astype(jnp.float32)
        for source in range(1, depth):
            own = own + line_in[source, y, x].astype(jnp.float32)
        line_sum[...] = own

    def second(k):
        span = slice_of(k)
        for t in range(layers):
            with jax.named_scope(f"first{k}_{t}"):
                drain(first_in.at[t, :, :, span_of(k)], first_recv.at[k * layers + t])
            if t % 2 == 0:
                own, came = parts[t, 1 - y, x, :, span], first_in[t, 1 - y, :, span]
            else:
                own, came = parts[t, y, 1 - x, :, span], first_in[t, 1 - x, :, span]
            relay[t, :, span] = (
                own.astype(jnp.float32) + came.astype(jnp.float32)
            ).astype(jnp.bfloat16)
            second_copy(k, t).start()

    def column(k):
        span = slice_of(k)
        for t in range(layers):
            with jax.named_scope(f"second{k}_{t}"):
                second_copy(k, t).wait_recv()
            came = first_in[t, y if t % 2 == 0 else x, :, span].astype(jnp.float32)
            value = (
                parts[t, y, x, :, span].astype(jnp.float32)
                + came
                + second_in[t, :, span].astype(jnp.float32)
            ).astype(jnp.bfloat16)
            column_part[t, :, span] = value
            for side in range(2):
                own = jnp.logical_and(layer(core, t) == z, core == side)

                @pl.when(jnp.logical_not(own))
                def _():
                    column_copy(k, t, side).start()

                @pl.when(own)
                def _():
                    column_in[z, span] = value[side]

    def target_of(layer_to, head):
        return layer_to * PLANE + y * 4 + head

    def reach(k):
        return layers + 1 if pieces[k][3] else depth

    def row_copy(k, layer_to, head):
        span = span_of(k)
        return pltpu.make_async_remote_copy(
            blocks.at[head, span], tp_out.at[me, span],
            row_send, row_recv.at[k * depth + z], **to(target_of(layer_to, head))
        )

    def update(k):
        span = slice_of(k)
        with jax.named_scope(f"column{k}"):
            if pieces[k][2]:
                for sources, here in ((depth - 1, worker == core), (depth, worker != core)):
                    @pl.when(here)
                    def _():
                        drain(column_in.at[pl.ds(0, sources), span_of(k)], column_recv.at[k])
                gradients = column_in[0, span].astype(jnp.float32)
                for source in range(1, depth):
                    gradients = gradients + column_in[source, span].astype(jnp.float32)
            else:
                drain(plane_in, plane_recv)
                gradients = line_sum[...]
                for source in range(3):
                    gradients = gradients + plane_in[source].astype(jnp.float32)
        news = []
        for head in range(heads):
            m_new, v_new, w_new = adam_update(
                gradients[:, head * head_size : (head + 1) * head_size],
                m_ref[span, head, :], v_ref[span, head, :], w_ref[span, head, :],
            )
            narrow = w_new.astype(jnp.bfloat16)
            blocks[head, span] = narrow
            news.append((m_new, v_new, w_new))
        for place in reversed(range(reach(k))):
            for head in range(heads):
                target = target_of(mirrored(place), head)

                @pl.when(target != me)
                def _():
                    row_copy(k, mirrored(place), head).start()

        tp_out[me, span] = blocks[lax.rem(q, 4), span]
        for head, (m_new, v_new, w_new) in enumerate(news):
            m_out[span, head, :] = m_new
            v_out[span, head, :] = v_new
            w_out[span, head, :] = w_new

    def group_copy(k, layer_from, device, send, recv):
        block = tp_out.at[pl.ds(layer_from * PLANE + y * 4, 4), span_of(k)]
        return pltpu.make_async_remote_copy(block, block, send, recv, **to(device))

    def forward(k, places, relayed):
        for place in places:
            layer_from = mirrored(place)
            arrived = row_recv.at[k * depth + layer_from]
            with jax.named_scope(f"row{k}_{place}"):
                if place < layers:
                    for slabs, here in ((3, inward == place), (4, inward != place)):
                        @pl.when(here)
                        def _():
                            drain(tp_out.at[pl.ds(0, slabs), span_of(k)], arrived)
                else:
                    drain(tp_out.at[pl.ds(0, 4), span_of(k)], arrived)
            if relayed:
                for other in range(layers - 1):
                    group_copy(
                        k, layer_from, mirrored(other) * PLANE + q, far_send, arrived
                    ).start()
            group_copy(k, layer_from, y_mate, side_send, side_recv).start()

    def near(k):
        forward(k, range(layers), False)

    def gate(k):
        @pl.when(inward == layers - 1)
        def _():
            forward(k, range(layers, depth), pieces[k][3])

    def end(k):
        @pl.when(inward != layers - 1)
        def _():
            forward(k, range(layers, depth), False)

    for t in range(layers):
        mate_part[t] = dot_tile(1 - core, t).astype(jnp.bfloat16)
        if t == 0:
            with jax.named_scope("barrier"):
                pl.semaphore_wait(
                    barrier, 4 + has_lower.astype(jnp.int32) + has_upper.astype(jnp.int32)
                )
            point(0)
        mate_copy(0, t).start()
        total[t] = dot_tile(core, t)
        if t:
            for k in range(1, len(pieces)):
                for other in range(layers):
                    mate_copy(k, other).start()

    for load in loads[2:]:
        load.wait()
    for action, k in ORDER:
        if action == "join":
            for t in range(layers):
                join(k, t)
        elif action == "point":
            with jax.named_scope(f"point{k}"):
                point(k)
        elif action == "second":
            second(k)
        elif action == "column":
            column(k)
        elif action == "across":
            across(k)
        elif action == "update":
            update(k)
        else:
            {"near": near, "gate": gate, "end": end}[action](k)

    with jax.named_scope("sends"):
        drain(mate_part, mate_send)
        for k in range(len(pieces)):
            span = span_of(k)
            if pieces[k][2]:
                drain(first_in.at[:, :, :, span], plane_send)
                drain(relay.at[:, :, span], plane_send)
            else:
                drain(plane_in, plane_send)
                for _ in range(layers * 2 - 1):
                    drain(plane_part, plane_send)

                @pl.when(worker != core)
                def _():
                    drain(plane_part, plane_send)
        for k in range(len(pieces)):
            if not pieces[k][2]:
                continue
            for sides, here in ((1, worker == core), (2, worker != core)):
                @pl.when(here)
                def _():
                    for t in range(layers):
                        drain(
                            column_part.at[t, pl.ds(0, sides if t == 0 else 2), span_of(k)],
                            column_send,
                        )
        for k in range(len(pieces)):
            drain(tp_out.at[pl.ds(0, heads * reach(k) - 1), span_of(k)], row_send)
            if pieces[k][3] and layers > 1:
                @pl.when(inward == layers - 1)
                def _():
                    for _ in range(layers - 1):
                        drain(tp_out.at[pl.ds(0, 4 * layers), span_of(k)], far_send)
        slabs = tp_out.at[pl.ds(0, depth * 4)]
        drain(slabs, side_send)
    with jax.named_scope("last"):
        drain(slabs, side_recv)


POINTS = 3
PARTS = ((16, True, True),) * 4 + ((16, False, True),)
ORDER = (
    ("join", 0), ("join", 1), ("join", 2), ("point", 1), ("point", 2), ("point", 3),
    ("join", 4), ("second", 0), ("join", 3), ("second", 1), ("second", 2), ("column", 0),
    ("second", 3), ("column", 1), ("column", 2), ("update", 0), ("column", 3), ("across", 4),
    ("update", 1), ("near", 0), ("update", 4), ("gate", 0), ("update", 2), ("near", 1),
    ("update", 3), ("gate", 1), ("near", 4), ("gate", 4), ("end", 0), ("near", 2), ("gate", 2),
    ("near", 3), ("gate", 3), ("end", 1), ("end", 4), ("end", 2), ("end", 3),
)


def row_pieces(rows):
    pieces, start = [], 0
    for i, (share, twice, deputed) in enumerate(PARTS):
        count = rows - start if i + 1 == len(PARTS) else share
        pieces.append((start, count, twice, deputed))
        start += count
    return tuple(pieces)


def finish_kernel(*refs):
    count = (len(refs) - 1) // 2
    copies = [
        pltpu.make_async_copy(refs[i], refs[count + i], refs[-1].at[i])
        for i in range(count)
    ]
    for copy in copies:
        copy.start()
    for copy in copies:
        copy.wait()


def fused(n, inputs, value_cotangent, master, first_moment, second_moment):
    tokens, features = inputs.shape
    width = value_cotangent.shape[1]
    rows, heads, head_size = master.shape
    depth = n // PLANE
    layers = depth // 2
    pieces = row_pieces(rows)
    state = jax.ShapeDtypeStruct(master.shape, jnp.float32)
    slabs = jax.ShapeDtypeStruct((n, rows, head_size), jnp.bfloat16)
    block = jax.ShapeDtypeStruct((1, features, head_size), jnp.bfloat16)
    results = 12 * master.size + 2 * block.size + SPARE_BYTES
    vmem = pl.BlockSpec(memory_space=pltpu.VMEM)
    narrow = jnp.bfloat16
    dma = pltpu.SemaphoreType.DMA
    held = pl.pallas_call(
        functools.partial(step_kernel, n, pieces),
        out_shape=tuple(pltpu.VMEM(a.shape, a.dtype) for a in (state, state, state, slabs)),
        in_specs=[pl.BlockSpec(memory_space=pltpu.HBM)] * 5,
        out_specs=[vmem] * 4,
        scratch_shapes=[
            pltpu.VMEM((tokens, features), narrow),
            pltpu.VMEM((tokens, width), narrow),
            pltpu.VMEM(master.shape, jnp.float32),
            pltpu.VMEM(master.shape, jnp.float32),
            pltpu.VMEM(master.shape, jnp.float32),
            pltpu.VMEM((layers, 2, 2, 2, rows, width), jnp.float32),
            pltpu.VMEM((layers, 2, 2, 2, rows, width), narrow),
            pltpu.VMEM((layers, 2, 2, 2, rows, width), narrow),
            pltpu.VMEM((layers, 2, 2, 2, rows, width), narrow),
            pltpu.VMEM((layers, 2, 2, rows, width), narrow),
            pltpu.VMEM((layers, 2, rows, width), narrow),
            pltpu.VMEM((layers, 2, rows, width), narrow),
            pltpu.VMEM((layers, 2, rows, width), narrow),
            pltpu.VMEM((depth, rows, width), narrow),
            pltpu.VMEM((depth, 2, 2, pieces[-1][1], width), narrow),
            pltpu.VMEM((pieces[-1][1], width), jnp.float32),
            pltpu.VMEM((2, 2, pieces[-1][1], width), narrow),
            pltpu.VMEM((3, pieces[-1][1], width), narrow),
            pltpu.VMEM((heads, rows, head_size), narrow),
            dma((5,)),
            dma,
            dma((layers * len(pieces),)),
            dma,
            dma((layers * len(pieces),)),
            dma((layers * len(pieces),)),
            dma,
            dma((len(pieces),)),
            dma,
            dma((depth * len(pieces),)),
            dma,
            dma,
            dma,
            dma,
            dma,
            pltpu.SemaphoreType.REGULAR,
            pltpu.SemaphoreType.REGULAR,
        ],
        compiler_params=pltpu.CompilerParams(
            collective_id=0, has_side_effects=True, vmem_limit_bytes=VMEM_BYTES - results
        ),
    )(inputs, value_cotangent, master, first_moment, second_moment)
    held = held[:3] + (held[3].reshape(block.shape),)
    return pl.pallas_call(
        finish_kernel,
        out_shape=(state, state, state, block),
        in_specs=[vmem] * 4,
        out_specs=[pl.BlockSpec(memory_space=pltpu.HBM)] * 4,
        scratch_shapes=[dma((4,))],
        compiler_params=pltpu.CompilerParams(vmem_limit_bytes=VMEM_BYTES // 2),
    )(*held)


def solution(mesh):
    n = mesh.shape["fsdp"]

    def body(inputs, value_cotangent, master, first_moment, second_moment):
        rows = master.shape[0]
        direct = (
            mesh.shape["dp"] == 1
            and n % (2 * PLANE) == 0
            and inputs.shape[1] % (256 * (n // (2 * PLANE))) == 0
            and rows % 16 == 0
            and rows > sum(part[0] for part in PARTS[:-1])
            and master.shape[1] * 2 == PLANE
            and master.shape[2] % 128 == 0
        )
        if direct:
            return fused(n, inputs, value_cotangent, master, first_moment, second_moment)
        return shards(inputs, value_cotangent, master, first_moment, second_moment)

    placed = (
        P(("fsdp", "dp"), None),
        P(("fsdp", "dp"), None),
        P("fsdp", None, "dp"),
        P("fsdp", None, "dp"),
        P("fsdp", None, "dp"),
    )
    return jax.shard_map(
        body,
        mesh=mesh,
        in_specs=placed,
        out_specs=(
            P("fsdp", None, "dp"),
            P("fsdp", None, "dp"),
            P("fsdp", None, "dp"),
            P("fsdp", None, "dp"),
        ),
        check_vma=False,
    )
```

```python
import functools

import jax
import jax.numpy as jnp
from jax import lax
from jax.experimental import pallas as pl
from jax.experimental.pallas import tpu as pltpu
from jax.sharding import PartitionSpec as P

STEP = 8


beta_first = 0.9
beta_second = 0.95
learn_rate = 0.001
weight_decay = 0.1
epsilon = 1e-08


def adam_update(gradient, moment_one, moment_two, weights):
    moment_one_new = beta_first * moment_one + (1.0 - beta_first) * gradient
    moment_two_new = beta_second * moment_two + (1.0 - beta_second) * gradient * gradient
    correct_one = 1.0 - beta_first**STEP
    correct_two = 1.0 - beta_second**STEP
    update = (
        moment_one_new / correct_one / (jnp.sqrt(moment_two_new / correct_two) + epsilon)
        + weight_decay * weights
    )
    return (moment_one_new, moment_two_new, weights - learn_rate * update)


def shards(inputs, value_cotangent, master, first_moment, second_moment):
    _, heads, slice_width = master.shape
    head_size = value_cotangent.shape[1] // heads
    head_parts = []
    for head in range(heads):
        head_cot = value_cotangent[:, head * head_size : (head + 1) * head_size]
        head_term = lax.dot_general(
            inputs, head_cot, (((0,), (0,)), ((), ())), preferred_element_type=jnp.float32
        )
        head_parts.append(
            lax.psum_scatter(
                head_term.astype(jnp.bfloat16), "dp", scatter_dimension=1, tiled=True
            ).astype(jnp.float32)
        )
    column_part = jnp.stack(head_parts, axis=1)
    grad_share = lax.psum_scatter(column_part, "fsdp", scatter_dimension=0, tiled=True)
    moment_one_new, moment_two_new, master_new = adam_update(
        grad_share, first_moment, second_moment, master
    )
    narrow_weight = master_new.astype(jnp.bfloat16)
    gathered = lax.all_gather(narrow_weight, "fsdp", axis=0, tiled=True)
    head_index = lax.axis_index("fsdp") % heads
    picked = lax.dynamic_slice_in_dim(gathered, head_index, 1, 1)
    tp_block = picked.reshape(1, gathered.shape[0], slice_width)
    return (moment_one_new, moment_two_new, master_new, tp_block)


VMEM_BYTES = 67043328
SPARE_BYTES = 64 * 1024
PLANE = 8


def step_kernel(
    n, pieces, x_hbm, g_hbm, w_hbm, m_hbm, v_hbm, m_out, v_out, w_out, tp_out,
    x_ref, g_ref, w_ref, m_ref, v_ref,
    total, mate_part, mate_in, parts, first_in, relay, second_in,
    column_part, column_in, line_in, line_sum, plane_part, plane_in, blocks,
    load_sem, mate_send, mate_recv, plane_send, first_recv, second_recv,
    column_send, column_recv, row_send, row_recv, far_send, side_send, side_recv,
    line_recv, plane_recv, up_sem, down_sem,
):
    me = lax.axis_index("fsdp")
    z = me // PLANE
    q = lax.rem(me, PLANE)
    y = q // 4
    x = lax.rem(q // 2, 2)
    core = lax.rem(q, 2)
    mate = me + 1 - 2 * core
    x_mate = me + 2 - 4 * x
    y_mate = me + 4 - 8 * y
    xy_mate = x_mate + 4 - 8 * y
    depth = n // PLANE
    layers = depth // 2
    rows, heads, head_size = w_ref.shape
    half = x_ref.shape[1] // 2
    tile = half // layers
    worker = z // layers

    def mirrored(place):
        return place + worker * (depth - 1 - 2 * place)

    inward = mirrored(z)

    def layer(side, t):
        return t + side * (depth - 1 - 2 * t)

    def columns(side, t):
        return pl.ds(pl.multiple_of(layer(side, t) * tile, 128), tile)

    tiles = [(side, t) for side in (1 - core, core) for t in range(layers)]
    load_g = pltpu.make_async_copy(g_hbm, g_ref, load_sem.at[0])
    load_x = [
        pltpu.make_async_copy(
            x_hbm.at[:, columns(*place)], x_ref.at[:, columns(*place)], load_sem.at[4 + i]
        )
        for i, place in enumerate(tiles)
    ]
    load_state = [
        pltpu.make_async_copy(source, target, load_sem.at[1 + i])
        for i, (source, target) in enumerate(((w_hbm, w_ref), (m_hbm, m_ref), (v_hbm, v_ref)))
    ]
    load_g.start()
    for load in load_x + load_state:
        load.start()

    def to(device):
        return dict(device_id={"fsdp": device}, device_id_type=pl.DeviceIdType.MESH)

    barrier = pltpu.get_barrier_semaphore()
    for slot in range(4):
        @pl.when(lax.rem(q, 4) != slot)
        def _():
            pl.semaphore_signal(barrier, inc=1, **to(z * PLANE + y * 4 + slot))
    pl.semaphore_signal(barrier, inc=1, **to(y_mate))
    has_lower, has_upper = z > 0, z < depth - 1

    @pl.when(has_lower)
    def _():
        pl.semaphore_signal(barrier, inc=1, **to(me - PLANE))

    @pl.when(has_upper)
    def _():
        pl.semaphore_signal(barrier, inc=1, **to(me + PLANE))

    def point(p):
        for rank, behind, ahead, semaphore, step in (
            (z, has_lower, has_upper, up_sem, PLANE),
            (depth - 1 - z, has_upper, has_lower, down_sem, -PLANE),
        ):
            @pl.when(rank == p if p < POINTS else rank >= p)
            def _():
                @pl.when(behind)
                def _():
                    pl.semaphore_wait(semaphore, 1)

                @pl.when(ahead)
                def _():
                    pl.semaphore_signal(semaphore, inc=1, **to(me + step))

    def dot_tile(side, t):
        return lax.dot_general(
            x_ref[:, columns(side, t)], g_ref[...], (((0,), (0,)), ((), ())),
            preferred_element_type=jnp.float32,
        ).reshape(2, 2, 2, rows, heads * head_size)

    def span_of(k):
        start, count = pieces[k][:2]
        return pl.ds(start, count)

    def slice_of(k):
        start, count = pieces[k][:2]
        return slice(start, start + count)

    def mate_copy(k, t):
        span = span_of(k)
        return pltpu.make_async_remote_copy(
            mate_part.at[t, :, :, :, span], mate_in.at[t, :, :, :, span],
            mate_send, mate_recv.at[k * layers + t], **to(mate)
        )

    def first_copies(k, t):
        span = span_of(k)
        arrived = first_recv.at[k * layers + t]
        if t % 2 == 0:
            moves = ((parts.at[t, :, 1 - x, :, span], first_in.at[t, :, :, span], x_mate),)
        else:
            moves = ((parts.at[t, 1 - y, :, :, span], first_in.at[t, :, :, span], y_mate),)
        return [
            pltpu.make_async_remote_copy(source, target, plane_send, arrived, **to(device))
            for source, target, device in moves
        ]

    def second_copy(k, t):
        span = span_of(k)
        return pltpu.make_async_remote_copy(
            relay.at[t, :, span], second_in.at[t, :, span],
            plane_send, second_recv.at[k * layers + t],
            **to(y_mate if t % 2 == 0 else x_mate)
        )

    def column_copy(k, t, side):
        span = span_of(k)
        return pltpu.make_async_remote_copy(
            column_part.at[t, side, span], column_in.at[z, span],
            column_send, column_recv.at[k],
            **to(layer(core, t) * PLANE + 2 * (q // 2) + side),
        )

    def drain(block, semaphore):
        pltpu.make_async_copy(block, block, semaphore).wait()

    def join(k, t):
        span = slice_of(k)
        with jax.named_scope(f"mate{k}_{t}"):
            mate_copy(k, t).wait_recv()
        value = (
            total[t, :, :, :, span] + mate_in[t, :, :, :, span].astype(jnp.float32)
        ).astype(jnp.bfloat16)
        parts[t, :, :, :, span] = value
        if pieces[k][2]:
            for copy in first_copies(k, t):
                copy.start()
            return
        for side in range(2):
            own = jnp.logical_and(layer(core, t) == z, core == side)

            @pl.when(jnp.logical_not(own))
            def _():
                pltpu.make_async_remote_copy(
                    parts.at[t, :, :, side, span_of(k)], line_in.at[z], plane_send, line_recv,
                    **to(layer(core, t) * PLANE + 2 * (q // 2) + side)
                ).start()

            @pl.when(own)
            def _():
                line_in[z] = value[:, :, side]

    def across(k):
        with jax.named_scope(f"line{k}"):
            for sources, here in ((depth - 1, worker == core), (depth, worker != core)):
                @pl.when(here)
                def _():
                    drain(line_in.at[pl.ds(0, sources)], line_recv)
        value = line_in[0].astype(jnp.float32)
        for source in range(1, depth):
            value = value + line_in[source].astype(jnp.float32)
        plane_part[...] = value.astype(jnp.bfloat16)
        for slot, (row, column_at, device) in enumerate(
            ((y, 1 - x, x_mate), (1 - y, x, y_mate), (1 - y, 1 - x, xy_mate))
        ):
            pltpu.make_async_remote_copy(
                plane_part.at[row, column_at], plane_in.at[slot], plane_send, plane_recv,
                **to(device)
            ).start()
        own = line_in[0, y, x].astype(jnp.float32)
        for source in range(1, depth):
            own = own + line_in[source, y, x].astype(jnp.float32)
        line_sum[...] = own

    def second(k):
        span = slice_of(k)
        for t in range(layers):
            with jax.named_scope(f"first{k}_{t}"):
                drain(first_in.at[t, :, :, span_of(k)], first_recv.at[k * layers + t])
            if t % 2 == 0:
                own, came = parts[t, 1 - y, x, :, span], first_in[t, 1 - y, :, span]
            else:
                own, came = parts[t, y, 1 - x, :, span], first_in[t, 1 - x, :, span]
            relay[t, :, span] = (
                own.astype(jnp.float32) + came.astype(jnp.float32)
            ).astype(jnp.bfloat16)
            second_copy(k, t).start()

    def column(k):
        span = slice_of(k)
        for t in range(layers):
            with jax.named_scope(f"second{k}_{t}"):
                second_copy(k, t).wait_recv()
            came = first_in[t, y if t % 2 == 0 else x, :, span].astype(jnp.float32)
            value = (
                parts[t, y, x, :, span].astype(jnp.float32)
                + came
                + second_in[t, :, span].astype(jnp.float32)
            ).astype(jnp.bfloat16)
            column_part[t, :, span] = value
            for side in range(2):
                own = jnp.logical_and(layer(core, t) == z, core == side)

                @pl.when(jnp.logical_not(own))
                def _():
                    column_copy(k, t, side).start()

                @pl.when(own)
                def _():
                    column_in[z, span] = value[side]

    def target_of(layer_to, head):
        return layer_to * PLANE + y * 4 + head

    def reach(k):
        return layers + 1 if pieces[k][3] else depth

    def row_copy(k, layer_to, head):
        span = span_of(k)
        return pltpu.make_async_remote_copy(
            blocks.at[head, span], tp_out.at[me, span],
            row_send, row_recv.at[k * depth + z], **to(target_of(layer_to, head))
        )

    def update(k):
        span = slice_of(k)
        with jax.named_scope(f"column{k}"):
            if pieces[k][2]:
                for sources, here in ((depth - 1, worker == core), (depth, worker != core)):
                    @pl.when(here)
                    def _():
                        drain(column_in.at[pl.ds(0, sources), span_of(k)], column_recv.at[k])
                gradients = column_in[0, span].astype(jnp.float32)
                for source in range(1, depth):
                    gradients = gradients + column_in[source, span].astype(jnp.float32)
            else:
                drain(plane_in, plane_recv)
                gradients = line_sum[...]
                for source in range(3):
                    gradients = gradients + plane_in[source].astype(jnp.float32)
        news = []
        for head in range(heads):
            m_new, v_new, w_new = adam_update(
                gradients[:, head * head_size : (head + 1) * head_size],
                m_ref[span, head, :], v_ref[span, head, :], w_ref[span, head, :],
            )
            narrow = w_new.astype(jnp.bfloat16)
            blocks[head, span] = narrow
            news.append((m_new, v_new, w_new))
        for place in reversed(range(reach(k))):
            for head in range(heads):
                target = target_of(mirrored(place), head)

                @pl.when(target != me)
                def _():
                    row_copy(k, mirrored(place), head).start()

        for head in range(heads):
            pltpu.make_async_remote_copy(
                blocks.at[head, span_of(k)], tp_out.at[me, span_of(k)], row_send, side_recv,
                **to(z * PLANE + (1 - y) * 4 + head)
            ).start()
        tp_out[me, span] = blocks[lax.rem(q, 4), span]
        for head, (m_new, v_new, w_new) in enumerate(news):
            m_out[span, head, :] = m_new
            v_out[span, head, :] = v_new
            w_out[span, head, :] = w_new

    def group_copy(k, layer_from, device, send, recv):
        block = tp_out.at[pl.ds(layer_from * PLANE + y * 4, 4), span_of(k)]
        return pltpu.make_async_remote_copy(block, block, send, recv, **to(device))

    def forward(k, places, relayed, crossed):
        for place in places:
            layer_from = mirrored(place)
            arrived = row_recv.at[k * depth + layer_from]
            with jax.named_scope(f"row{k}_{place}"):
                if place < layers:
                    for slabs, here in ((3, inward == place), (4, inward != place)):
                        @pl.when(here)
                        def _():
                            drain(tp_out.at[pl.ds(0, slabs), span_of(k)], arrived)
                else:
                    drain(tp_out.at[pl.ds(0, 4), span_of(k)], arrived)
            for other in range(layers - 1 if relayed else 0):
                there = mirrored(other) * PLANE + q
                group_copy(k, layer_from, there, far_send, arrived).start()
                if relayed == 2:
                    group_copy(k, layer_from, there + y_mate - me, far_send, side_recv).start()
            if not crossed:
                continue
            if place >= layers:
                group_copy(k, layer_from, y_mate, side_send, side_recv).start()
            else:
                @pl.when(inward != place)
                def _():
                    group_copy(k, layer_from, y_mate, side_send, side_recv).start()

    def near(k):
        forward(k, range(layers), 0, True)

    def gate(k):
        @pl.when(inward == layers - 1)
        def _():
            forward(k, range(layers, depth), pieces[k][3], True)

    def end(k):
        @pl.when(inward != layers - 1)
        def _():
            forward(k, range(layers, depth), 0, pieces[k][3] != 2)

    with jax.named_scope("loads"):
        load_g.wait()
    for t in range(layers):
        with jax.named_scope(f"load{t}"):
            load_x[t].wait()
        mate_part[t] = dot_tile(1 - core, t).astype(jnp.bfloat16)
        if t == 0:
            with jax.named_scope("barrier"):
                pl.semaphore_wait(
                    barrier, 4 + has_lower.astype(jnp.int32) + has_upper.astype(jnp.int32)
                )
            point(0)
        mate_copy(0, t).start()
    for k in range(1, len(pieces)):
        for t in range(layers):
            mate_copy(k, t).start()
    for t in range(layers):
        load_x[layers + t].wait()
        total[t] = dot_tile(core, t)
    for load in load_state:
        load.wait()
    for action, k in ORDER:
        if action == "join":
            for t in range(layers):
                join(k, t)
        elif action == "point":
            with jax.named_scope(f"point{k}"):
                point(k)
        elif action == "second":
            second(k)
        elif action == "column":
            column(k)
        elif action == "across":
            across(k)
        elif action == "update":
            update(k)
        else:
            {"near": near, "gate": gate, "end": end}[action](k)

    with jax.named_scope("sends"):
        drain(mate_part, mate_send)
        for k in range(len(pieces)):
            span = span_of(k)
            if pieces[k][2]:
                drain(first_in.at[:, :, :, span], plane_send)
                drain(relay.at[:, :, span], plane_send)
            else:
                drain(plane_in, plane_send)
                for _ in range(layers * 2 - 1):
                    drain(plane_part, plane_send)

                @pl.when(worker != core)
                def _():
                    drain(plane_part, plane_send)
        for k in range(len(pieces)):
            if not pieces[k][2]:
                continue
            for sides, here in ((1, worker == core), (2, worker != core)):
                @pl.when(here)
                def _():
                    for t in range(layers):
                        drain(
                            column_part.at[t, pl.ds(0, sides if t == 0 else 2), span_of(k)],
                            column_send,
                        )
        for k in range(len(pieces)):
            drain(tp_out.at[pl.ds(0, heads * (reach(k) + 1) - 1), span_of(k)], row_send)
            if pieces[k][3] and layers > 1:
                @pl.when(inward == layers - 1)
                def _():
                    for _ in range((layers - 1) * pieces[k][3]):
                        drain(tp_out.at[pl.ds(0, 4 * layers), span_of(k)], far_send)
            for slabs, here in (
                ((depth - 1) * 4, inward == layers - 1),
                (((layers if pieces[k][3] == 2 else depth) - 1) * 4, inward != layers - 1),
            ):
                @pl.when(here)
                def _():
                    drain(tp_out.at[pl.ds(0, slabs), span_of(k)], side_send)
        slabs = tp_out.at[pl.ds(0, depth * 4)]
    with jax.named_scope("last"):
        drain(slabs, side_recv)


POINTS = 3
PARTS = ((16, True, 1), (16, True, 1), (16, True, 1), (16, True, 2), (16, False, 1))
ORDER = (
    ("join", 0), ("join", 1), ("join", 2), ("point", 1), ("point", 2), ("point", 3),
    ("join", 4), ("second", 0), ("join", 3), ("second", 1), ("second", 2), ("column", 0),
    ("second", 3), ("across", 4), ("column", 1), ("column", 2), ("update", 0), ("column", 3),
    ("update", 1), ("near", 0), ("update", 4), ("gate", 0), ("update", 2), ("near", 1),
    ("update", 3), ("gate", 1), ("near", 4), ("gate", 4), ("end", 0), ("near", 2), ("gate", 2),
    ("near", 3), ("gate", 3), ("end", 1), ("end", 4), ("end", 2), ("end", 3),
)


def row_pieces(rows):
    pieces, start = [], 0
    for i, (share, twice, deputed) in enumerate(PARTS):
        count = rows - start if i + 1 == len(PARTS) else share
        pieces.append((start, count, twice, deputed))
        start += count
    return tuple(pieces)


def finish_kernel(*refs):
    count = (len(refs) - 1) // 2
    copies = [
        pltpu.make_async_copy(refs[i], refs[count + i], refs[-1].at[i])
        for i in range(count)
    ]
    for copy in copies:
        copy.start()
    for copy in copies:
        copy.wait()


def fused(n, inputs, value_cotangent, master, first_moment, second_moment):
    tokens, features = inputs.shape
    width = value_cotangent.shape[1]
    rows, heads, head_size = master.shape
    depth = n // PLANE
    layers = depth // 2
    pieces = row_pieces(rows)
    state = jax.ShapeDtypeStruct(master.shape, jnp.float32)
    slabs = jax.ShapeDtypeStruct((n, rows, head_size), jnp.bfloat16)
    block = jax.ShapeDtypeStruct((1, features, head_size), jnp.bfloat16)
    results = 12 * master.size + 2 * block.size + SPARE_BYTES
    vmem = pl.BlockSpec(memory_space=pltpu.VMEM)
    narrow = jnp.bfloat16
    dma = pltpu.SemaphoreType.DMA
    held = pl.pallas_call(
        functools.partial(step_kernel, n, pieces),
        out_shape=tuple(pltpu.VMEM(a.shape, a.dtype) for a in (state, state, state, slabs)),
        in_specs=[pl.BlockSpec(memory_space=pltpu.HBM)] * 5,
        out_specs=[vmem] * 4,
        scratch_shapes=[
            pltpu.VMEM((tokens, features), narrow),
            pltpu.VMEM((tokens, width), narrow),
            pltpu.VMEM(master.shape, jnp.float32),
            pltpu.VMEM(master.shape, jnp.float32),
            pltpu.VMEM(master.shape, jnp.float32),
            pltpu.VMEM((layers, 2, 2, 2, rows, width), jnp.float32),
            pltpu.VMEM((layers, 2, 2, 2, rows, width), narrow),
            pltpu.VMEM((layers, 2, 2, 2, rows, width), narrow),
            pltpu.VMEM((layers, 2, 2, 2, rows, width), narrow),
            pltpu.VMEM((layers, 2, 2, rows, width), narrow),
            pltpu.VMEM((layers, 2, rows, width), narrow),
            pltpu.VMEM((layers, 2, rows, width), narrow),
            pltpu.VMEM((layers, 2, rows, width), narrow),
            pltpu.VMEM((depth, rows, width), narrow),
            pltpu.VMEM((depth, 2, 2, pieces[-1][1], width), narrow),
            pltpu.VMEM((pieces[-1][1], width), jnp.float32),
            pltpu.VMEM((2, 2, pieces[-1][1], width), narrow),
            pltpu.VMEM((3, pieces[-1][1], width), narrow),
            pltpu.VMEM((heads, rows, head_size), narrow),
            dma((4 + 2 * layers,)),
            dma,
            dma((layers * len(pieces),)),
            dma,
            dma((layers * len(pieces),)),
            dma((layers * len(pieces),)),
            dma,
            dma((len(pieces),)),
            dma,
            dma((depth * len(pieces),)),
            dma,
            dma,
            dma,
            dma,
            dma,
            pltpu.SemaphoreType.REGULAR,
            pltpu.SemaphoreType.REGULAR,
        ],
        compiler_params=pltpu.CompilerParams(
            collective_id=0, has_side_effects=True, vmem_limit_bytes=VMEM_BYTES - results
        ),
    )(inputs, value_cotangent, master, first_moment, second_moment)
    held = held[:3] + (held[3].reshape(block.shape),)
    return pl.pallas_call(
        finish_kernel,
        out_shape=(state, state, state, block),
        in_specs=[vmem] * 4,
        out_specs=[pl.BlockSpec(memory_space=pltpu.HBM)] * 4,
        scratch_shapes=[dma((4,))],
        compiler_params=pltpu.CompilerParams(vmem_limit_bytes=VMEM_BYTES // 2),
    )(*held)


def solution(mesh):
    n = mesh.shape["fsdp"]

    def body(inputs, value_cotangent, master, first_moment, second_moment):
        rows = master.shape[0]
        direct = (
            mesh.shape["dp"] == 1
            and n % (2 * PLANE) == 0
            and inputs.shape[1] % (256 * (n // (2 * PLANE))) == 0
            and rows % 16 == 0
            and rows > sum(part[0] for part in PARTS[:-1])
            and master.shape[1] * 2 == PLANE
            and master.shape[2] % 128 == 0
        )
        if direct:
            return fused(n, inputs, value_cotangent, master, first_moment, second_moment)
        return shards(inputs, value_cotangent, master, first_moment, second_moment)

    placed = (
        P(("fsdp", "dp"), None),
        P(("fsdp", "dp"), None),
        P("fsdp", None, "dp"),
        P("fsdp", None, "dp"),
        P("fsdp", None, "dp"),
    )
    return jax.shard_map(
        body,
        mesh=mesh,
        in_specs=placed,
        out_specs=(
            P("fsdp", None, "dp"),
            P("fsdp", None, "dp"),
            P("fsdp", None, "dp"),
            P("fsdp", None, "dp"),
        ),
        check_vma=False,
    )
```

```python
import functools

import jax
import jax.numpy as jnp
from jax import lax
from jax.experimental import pallas as pl
from jax.experimental.pallas import tpu as pltpu
from jax.sharding import PartitionSpec as P

STEP = 8


beta_first = 0.9
beta_second = 0.95
learn_rate = 0.001
weight_decay = 0.1
epsilon = 1e-08


def adam_update(gradient, moment_one, moment_two, weights):
    moment_one_new = beta_first * moment_one + (1.0 - beta_first) * gradient
    moment_two_new = beta_second * moment_two + (1.0 - beta_second) * gradient * gradient
    correct_one = 1.0 - beta_first**STEP
    correct_two = 1.0 - beta_second**STEP
    update = (
        moment_one_new / correct_one / (jnp.sqrt(moment_two_new / correct_two) + epsilon)
        + weight_decay * weights
    )
    return (moment_one_new, moment_two_new, weights - learn_rate * update)


def shards(inputs, value_cotangent, master, first_moment, second_moment):
    _, heads, slice_width = master.shape
    head_size = value_cotangent.shape[1] // heads
    head_parts = []
    for head in range(heads):
        head_cot = value_cotangent[:, head * head_size : (head + 1) * head_size]
        head_term = lax.dot_general(
            inputs, head_cot, (((0,), (0,)), ((), ())), preferred_element_type=jnp.float32
        )
        head_parts.append(
            lax.psum_scatter(
                head_term.astype(jnp.bfloat16), "dp", scatter_dimension=1, tiled=True
            ).astype(jnp.float32)
        )
    column_part = jnp.stack(head_parts, axis=1)
    grad_share = lax.psum_scatter(column_part, "fsdp", scatter_dimension=0, tiled=True)
    moment_one_new, moment_two_new, master_new = adam_update(
        grad_share, first_moment, second_moment, master
    )
    narrow_weight = master_new.astype(jnp.bfloat16)
    gathered = lax.all_gather(narrow_weight, "fsdp", axis=0, tiled=True)
    head_index = lax.axis_index("fsdp") % heads
    picked = lax.dynamic_slice_in_dim(gathered, head_index, 1, 1)
    tp_block = picked.reshape(1, gathered.shape[0], slice_width)
    return (moment_one_new, moment_two_new, master_new, tp_block)


VMEM_BYTES = 67043328
SPARE_BYTES = 64 * 1024
PLANE = 8


def step_kernel(
    n, pieces, x_hbm, g_hbm, w_hbm, m_hbm, v_hbm, m_out, v_out, w_out, tp_out,
    x_ref, g_ref, w_ref, m_ref, v_ref,
    total, mate_part, mate_in, parts, first_in, relay, second_in,
    column_part, column_in, line_in, line_sum, plane_part, plane_in, blocks,
    load_sem, mate_send, mate_recv, plane_send, first_recv, second_recv,
    column_send, column_recv, row_send, row_recv, far_send, side_send, side_recv,
    line_recv, plane_recv, up_sem, down_sem,
):
    me = lax.axis_index("fsdp")
    z = me // PLANE
    q = lax.rem(me, PLANE)
    y = q // 4
    x = lax.rem(q // 2, 2)
    core = lax.rem(q, 2)
    mate = me + 1 - 2 * core
    x_mate = me + 2 - 4 * x
    y_mate = me + 4 - 8 * y
    xy_mate = x_mate + 4 - 8 * y
    depth = n // PLANE
    layers = depth // 2
    rows, heads, head_size = w_ref.shape
    half = x_ref.shape[1] // 2
    tile = half // layers
    worker = z // layers

    def mirrored(place):
        return place + worker * (depth - 1 - 2 * place)

    inward = mirrored(z)

    def layer(side, t):
        return t + side * (depth - 1 - 2 * t)

    def columns(side, t):
        return pl.ds(pl.multiple_of(layer(side, t) * tile, 128), tile)

    tiles = [(side, t) for side in (1 - core, core) for t in range(layers)]
    load_g = pltpu.make_async_copy(g_hbm, g_ref, load_sem.at[0])
    load_x = [
        pltpu.make_async_copy(
            x_hbm.at[:, columns(*place)], x_ref.at[:, columns(*place)], load_sem.at[2 + i]
        )
        for i, place in enumerate(tiles)
    ]
    load_state = [
        pltpu.make_async_copy(source, target, load_sem.at[1])
        for source, target in ((w_hbm, w_ref), (m_hbm, m_ref), (v_hbm, v_ref))
    ]
    load_g.start()
    for load in load_x + load_state:
        load.start()

    def to(device):
        return dict(device_id={"fsdp": device}, device_id_type=pl.DeviceIdType.MESH)

    barrier = pltpu.get_barrier_semaphore()
    for slot in range(4):
        @pl.when(lax.rem(q, 4) != slot)
        def _():
            pl.semaphore_signal(barrier, inc=1, **to(z * PLANE + y * 4 + slot))
    pl.semaphore_signal(barrier, inc=1, **to(y_mate))
    has_lower, has_upper = z > 0, z < depth - 1

    @pl.when(has_lower)
    def _():
        pl.semaphore_signal(barrier, inc=1, **to(me - PLANE))

    @pl.when(has_upper)
    def _():
        pl.semaphore_signal(barrier, inc=1, **to(me + PLANE))

    def point(p):
        for rank, behind, ahead, semaphore, step in (
            (z, has_lower, has_upper, up_sem, PLANE),
            (depth - 1 - z, has_upper, has_lower, down_sem, -PLANE),
        ):
            @pl.when(rank == p if p < POINTS else rank >= p)
            def _():
                @pl.when(behind)
                def _():
                    pl.semaphore_wait(semaphore, 1)

                @pl.when(ahead)
                def _():
                    pl.semaphore_signal(semaphore, inc=1, **to(me + step))

    def dot_tile(side, t):
        return lax.dot_general(
            x_ref[:, columns(side, t)], g_ref[...], (((0,), (0,)), ((), ())),
            preferred_element_type=jnp.float32,
        ).reshape(2, 2, 2, rows, heads * head_size)

    def span_of(k):
        start, count = pieces[k][:2]
        return pl.ds(start, count)

    def slice_of(k):
        start, count = pieces[k][:2]
        return slice(start, start + count)

    def mate_copy(k, t):
        span = span_of(k)
        return pltpu.make_async_remote_copy(
            mate_part.at[t, :, :, :, span], mate_in.at[t, :, :, :, span],
            mate_send, mate_recv.at[k * layers + t], **to(mate)
        )

    def first_copies(k, t):
        span = span_of(k)
        arrived = first_recv.at[k * layers + t]
        if t % 2 == 0:
            moves = ((parts.at[t, :, 1 - x, :, span], first_in.at[t, :, :, span], x_mate),)
        else:
            moves = ((parts.at[t, 1 - y, :, :, span], first_in.at[t, :, :, span], y_mate),)
        return [
            pltpu.make_async_remote_copy(source, target, plane_send, arrived, **to(device))
            for source, target, device in moves
        ]

    def second_copy(k, t):
        span = span_of(k)
        return pltpu.make_async_remote_copy(
            relay.at[t, :, span], second_in.at[t, :, span],
            plane_send, second_recv.at[k * layers + t],
            **to(y_mate if t % 2 == 0 else x_mate)
        )

    def column_copy(k, t, side):
        span = span_of(k)
        return pltpu.make_async_remote_copy(
            column_part.at[t, side, span], column_in.at[z, span],
            column_send, column_recv.at[k],
            **to(layer(core, t) * PLANE + 2 * (q // 2) + side),
        )

    def drain(block, semaphore):
        pltpu.make_async_copy(block, block, semaphore).wait()

    def join(k, t):
        span = slice_of(k)
        with jax.named_scope(f"mate{k}_{t}"):
            mate_copy(k, t).wait_recv()
        value = (
            total[t, :, :, :, span] + mate_in[t, :, :, :, span].astype(jnp.float32)
        ).astype(jnp.bfloat16)
        parts[t, :, :, :, span] = value
        if pieces[k][2]:
            for copy in first_copies(k, t):
                copy.start()
            return
        for side in range(2):
            own = jnp.logical_and(layer(core, t) == z, core == side)

            @pl.when(jnp.logical_not(own))
            def _():
                pltpu.make_async_remote_copy(
                    parts.at[t, :, :, side, span_of(k)], line_in.at[z], plane_send, line_recv,
                    **to(layer(core, t) * PLANE + 2 * (q // 2) + side)
                ).start()

            @pl.when(own)
            def _():
                line_in[z] = value[:, :, side]

    def across(k):
        with jax.named_scope(f"line{k}"):
            for sources, here in ((depth - 1, worker == core), (depth, worker != core)):
                @pl.when(here)
                def _():
                    drain(line_in.at[pl.ds(0, sources)], line_recv)
        value = line_in[0].astype(jnp.float32)
        for source in range(1, depth):
            value = value + line_in[source].astype(jnp.float32)
        plane_part[...] = value.astype(jnp.bfloat16)
        for slot, (row, column_at, device) in enumerate(
            ((y, 1 - x, x_mate), (1 - y, x, y_mate), (1 - y, 1 - x, xy_mate))
        ):
            pltpu.make_async_remote_copy(
                plane_part.at[row, column_at], plane_in.at[slot], plane_send, plane_recv,
                **to(device)
            ).start()
        own = line_in[0, y, x].astype(jnp.float32)
        for source in range(1, depth):
            own = own + line_in[source, y, x].astype(jnp.float32)
        line_sum[...] = own

    def second(k):
        span = slice_of(k)
        for t in range(layers):
            with jax.named_scope(f"first{k}_{t}"):
                drain(first_in.at[t, :, :, span_of(k)], first_recv.at[k * layers + t])
            if t % 2 == 0:
                own, came = parts[t, 1 - y, x, :, span], first_in[t, 1 - y, :, span]
            else:
                own, came = parts[t, y, 1 - x, :, span], first_in[t, 1 - x, :, span]
            relay[t, :, span] = (
                own.astype(jnp.float32) + came.astype(jnp.float32)
            ).astype(jnp.bfloat16)
            second_copy(k, t).start()

    def column(k):
        span = slice_of(k)
        for t in range(layers):
            with jax.named_scope(f"second{k}_{t}"):
                second_copy(k, t).wait_recv()
            came = first_in[t, y if t % 2 == 0 else x, :, span].astype(jnp.float32)
            value = (
                parts[t, y, x, :, span].astype(jnp.float32)
                + came
                + second_in[t, :, span].astype(jnp.float32)
            ).astype(jnp.bfloat16)
            column_part[t, :, span] = value
            for side in range(2):
                own = jnp.logical_and(layer(core, t) == z, core == side)

                @pl.when(jnp.logical_not(own))
                def _():
                    column_copy(k, t, side).start()

                @pl.when(own)
                def _():
                    column_in[z, span] = value[side]

    def target_of(layer_to, head):
        return layer_to * PLANE + y * 4 + head

    def reach(k):
        return layers + 1 if pieces[k][3] else depth

    def row_copy(k, layer_to, head):
        span = span_of(k)
        return pltpu.make_async_remote_copy(
            blocks.at[head, span], tp_out.at[me, span],
            row_send, row_recv.at[k * depth + z], **to(target_of(layer_to, head))
        )

    def update(k):
        span = slice_of(k)
        with jax.named_scope(f"column{k}"):
            if pieces[k][2]:
                for sources, here in ((depth - 1, worker == core), (depth, worker != core)):
                    @pl.when(here)
                    def _():
                        drain(column_in.at[pl.ds(0, sources), span_of(k)], column_recv.at[k])
                gradients = column_in[0, span].astype(jnp.float32)
                for source in range(1, depth):
                    gradients = gradients + column_in[source, span].astype(jnp.float32)
            else:
                drain(plane_in, plane_recv)
                gradients = line_sum[...]
                for source in range(3):
                    gradients = gradients + plane_in[source].astype(jnp.float32)
        news = []
        for head in range(heads):
            m_new, v_new, w_new = adam_update(
                gradients[:, head * head_size : (head + 1) * head_size],
                m_ref[span, head, :], v_ref[span, head, :], w_ref[span, head, :],
            )
            narrow = w_new.astype(jnp.bfloat16)
            blocks[head, span] = narrow
            news.append((m_new, v_new, w_new))
        for place in reversed(range(reach(k))):
            for head in range(heads):
                target = target_of(mirrored(place), head)

                @pl.when(target != me)
                def _():
                    row_copy(k, mirrored(place), head).start()

        for head in range(heads):
            pltpu.make_async_remote_copy(
                blocks.at[head, span_of(k)], tp_out.at[me, span_of(k)], row_send, side_recv,
                **to(z * PLANE + (1 - y) * 4 + head)
            ).start()
        tp_out[me, span] = blocks[lax.rem(q, 4), span]
        for head, (m_new, v_new, w_new) in enumerate(news):
            m_out[span, head, :] = m_new
            v_out[span, head, :] = v_new
            w_out[span, head, :] = w_new

    def group_copy(k, layer_from, device, send, recv):
        block = tp_out.at[pl.ds(layer_from * PLANE + y * 4, 4), span_of(k)]
        return pltpu.make_async_remote_copy(block, block, send, recv, **to(device))

    def forward(k, places, relayed, crossed):
        for place in places:
            layer_from = mirrored(place)
            arrived = row_recv.at[k * depth + layer_from]
            with jax.named_scope(f"row{k}_{place}"):
                if place < layers:
                    for slabs, here in ((3, inward == place), (4, inward != place)):
                        @pl.when(here)
                        def _():
                            drain(tp_out.at[pl.ds(0, slabs), span_of(k)], arrived)
                else:
                    drain(tp_out.at[pl.ds(0, 4), span_of(k)], arrived)
            for other in range(layers - 1 if relayed else 0):
                there = mirrored(other) * PLANE + q
                group_copy(k, layer_from, there, far_send, arrived).start()
                if relayed == 2:
                    group_copy(k, layer_from, there + y_mate - me, far_send, side_recv).start()
            if not crossed:
                continue
            if place >= layers:
                group_copy(k, layer_from, y_mate, side_send, side_recv).start()
            else:
                @pl.when(inward != place)
                def _():
                    group_copy(k, layer_from, y_mate, side_send, side_recv).start()

    def near(k):
        forward(k, range(layers), 0, True)

    def gate(k):
        @pl.when(inward == layers - 1)
        def _():
            forward(k, range(layers, depth), pieces[k][3], True)

    def end(k):
        @pl.when(inward != layers - 1)
        def _():
            forward(k, range(layers, depth), 0, pieces[k][3] != 2)

    with jax.named_scope("loads"):
        load_g.wait()
    for t in range(layers):
        with jax.named_scope(f"load{t}"):
            load_x[t].wait()
        mate_part[t] = dot_tile(1 - core, t).astype(jnp.bfloat16)
        if t == 0:
            with jax.named_scope("barrier"):
                pl.semaphore_wait(
                    barrier, 4 + has_lower.astype(jnp.int32) + has_upper.astype(jnp.int32)
                )
            point(0)
        mate_copy(0, t).start()
    for k in range(1, len(pieces)):
        for t in range(layers):
            mate_copy(k, t).start()
    for t in range(layers):
        load_x[layers + t].wait()
        total[t] = dot_tile(core, t)
    for load in load_state:
        load.wait()
    for action, k in ORDER:
        if action == "join":
            for t in range(layers):
                join(k, t)
        elif action == "point":
            with jax.named_scope(f"point{k}"):
                point(k)
        elif action == "second":
            second(k)
        elif action == "column":
            column(k)
        elif action == "across":
            across(k)
        elif action == "update":
            update(k)
        else:
            {"near": near, "gate": gate, "end": end}[action](k)

    with jax.named_scope("sends"):
        drain(mate_part, mate_send)
        for k in range(len(pieces)):
            span = span_of(k)
            if pieces[k][2]:
                drain(first_in.at[:, :, :, span], plane_send)
                drain(relay.at[:, :, span], plane_send)
            else:
                drain(plane_in, plane_send)
                for _ in range(layers * 2 - 1):
                    drain(plane_part, plane_send)

                @pl.when(worker != core)
                def _():
                    drain(plane_part, plane_send)
        for k in range(len(pieces)):
            if not pieces[k][2]:
                continue
            for sides, here in ((1, worker == core), (2, worker != core)):
                @pl.when(here)
                def _():
                    for t in range(layers):
                        drain(
                            column_part.at[t, pl.ds(0, sides if t == 0 else 2), span_of(k)],
                            column_send,
                        )
        for k in range(len(pieces)):
            drain(tp_out.at[pl.ds(0, heads * (reach(k) + 1) - 1), span_of(k)], row_send)
            if pieces[k][3] and layers > 1:
                @pl.when(inward == layers - 1)
                def _():
                    for _ in range((layers - 1) * pieces[k][3]):
                        drain(tp_out.at[pl.ds(0, 4 * layers), span_of(k)], far_send)
            for slabs, here in (
                ((depth - 1) * 4, inward == layers - 1),
                (((layers if pieces[k][3] == 2 else depth) - 1) * 4, inward != layers - 1),
            ):
                @pl.when(here)
                def _():
                    drain(tp_out.at[pl.ds(0, slabs), span_of(k)], side_send)
        slabs = tp_out.at[pl.ds(0, depth * 4)]
    with jax.named_scope("last"):
        drain(slabs, side_recv)


POINTS = 3
PARTS = ((16, True, 1), (16, True, 1), (16, True, 1), (16, True, 2), (16, False, 1))
ORDER = (
    ("join", 0), ("join", 1), ("join", 2), ("point", 1), ("point", 2), ("point", 3),
    ("join", 4), ("second", 0), ("join", 3), ("second", 1), ("second", 2), ("column", 0),
    ("second", 3), ("column", 1), ("across", 4), ("column", 2), ("update", 0), ("column", 3),
    ("update", 1), ("near", 0), ("update", 4), ("gate", 0), ("update", 2), ("near", 1),
    ("update", 3), ("gate", 1), ("near", 4), ("gate", 4), ("end", 0), ("near", 2), ("gate", 2),
    ("near", 3), ("gate", 3), ("end", 1), ("end", 4), ("end", 2), ("end", 3),
)


def row_pieces(rows):
    pieces, start = [], 0
    for i, (share, twice, deputed) in enumerate(PARTS):
        count = rows - start if i + 1 == len(PARTS) else share
        pieces.append((start, count, twice, deputed))
        start += count
    return tuple(pieces)


def finish_kernel(*refs):
    count = (len(refs) - 1) // 2
    copies = [
        pltpu.make_async_copy(refs[i], refs[count + i], refs[-1].at[i])
        for i in range(count)
    ]
    for copy in copies:
        copy.start()
    for copy in copies:
        copy.wait()


def fused(n, inputs, value_cotangent, master, first_moment, second_moment):
    tokens, features = inputs.shape
    width = value_cotangent.shape[1]
    rows, heads, head_size = master.shape
    depth = n // PLANE
    layers = depth // 2
    pieces = row_pieces(rows)
    state = jax.ShapeDtypeStruct(master.shape, jnp.float32)
    slabs = jax.ShapeDtypeStruct((n, rows, head_size), jnp.bfloat16)
    block = jax.ShapeDtypeStruct((1, features, head_size), jnp.bfloat16)
    results = 12 * master.size + 2 * block.size + SPARE_BYTES
    vmem = pl.BlockSpec(memory_space=pltpu.VMEM)
    narrow = jnp.bfloat16
    dma = pltpu.SemaphoreType.DMA
    held = pl.pallas_call(
        functools.partial(step_kernel, n, pieces),
        out_shape=tuple(pltpu.VMEM(a.shape, a.dtype) for a in (state, state, state, slabs)),
        in_specs=[pl.BlockSpec(memory_space=pltpu.HBM)] * 5,
        out_specs=[vmem] * 4,
        scratch_shapes=[
            pltpu.VMEM((tokens, features), narrow),
            pltpu.VMEM((tokens, width), narrow),
            pltpu.VMEM(master.shape, jnp.float32),
            pltpu.VMEM(master.shape, jnp.float32),
            pltpu.VMEM(master.shape, jnp.float32),
            pltpu.VMEM((layers, 2, 2, 2, rows, width), jnp.float32),
            pltpu.VMEM((layers, 2, 2, 2, rows, width), narrow),
            pltpu.VMEM((layers, 2, 2, 2, rows, width), narrow),
            pltpu.VMEM((layers, 2, 2, 2, rows, width), narrow),
            pltpu.VMEM((layers, 2, 2, rows, width), narrow),
            pltpu.VMEM((layers, 2, rows, width), narrow),
            pltpu.VMEM((layers, 2, rows, width), narrow),
            pltpu.VMEM((layers, 2, rows, width), narrow),
            pltpu.VMEM((depth, rows, width), narrow),
            pltpu.VMEM((depth, 2, 2, pieces[-1][1], width), narrow),
            pltpu.VMEM((pieces[-1][1], width), jnp.float32),
            pltpu.VMEM((2, 2, pieces[-1][1], width), narrow),
            pltpu.VMEM((3, pieces[-1][1], width), narrow),
            pltpu.VMEM((heads, rows, head_size), narrow),
            dma((2 + 2 * layers,)),
            dma,
            dma((layers * len(pieces),)),
            dma,
            dma((layers * (len(pieces) - 1),)),
            dma((layers * (len(pieces) - 1),)),
            dma,
            dma((len(pieces) - 1,)),
            dma,
            dma((depth * len(pieces),)),
            dma,
            dma,
            dma,
            dma,
            dma,
            pltpu.SemaphoreType.REGULAR,
            pltpu.SemaphoreType.REGULAR,
        ],
        compiler_params=pltpu.CompilerParams(
            collective_id=0, has_side_effects=True, vmem_limit_bytes=VMEM_BYTES - results
        ),
    )(inputs, value_cotangent, master, first_moment, second_moment)
    held = held[:3] + (held[3].reshape(block.shape),)
    return pl.pallas_call(
        finish_kernel,
        out_shape=(state, state, state, block),
        in_specs=[vmem] * 4,
        out_specs=[pl.BlockSpec(memory_space=pltpu.HBM)] * 4,
        scratch_shapes=[dma((4,))],
        compiler_params=pltpu.CompilerParams(vmem_limit_bytes=VMEM_BYTES // 2),
    )(*held)


def solution(mesh):
    n = mesh.shape["fsdp"]

    def body(inputs, value_cotangent, master, first_moment, second_moment):
        rows = master.shape[0]
        direct = (
            mesh.shape["dp"] == 1
            and n % (2 * PLANE) == 0
            and inputs.shape[1] % (256 * (n // (2 * PLANE))) == 0
            and rows % 16 == 0
            and rows > sum(part[0] for part in PARTS[:-1])
            and master.shape[1] * 2 == PLANE
            and master.shape[2] % 128 == 0
        )
        if direct:
            return fused(n, inputs, value_cotangent, master, first_moment, second_moment)
        return shards(inputs, value_cotangent, master, first_moment, second_moment)

    placed = (
        P(("fsdp", "dp"), None),
        P(("fsdp", "dp"), None),
        P("fsdp", None, "dp"),
        P("fsdp", None, "dp"),
        P("fsdp", None, "dp"),
    )
    return jax.shard_map(
        body,
        mesh=mesh,
        in_specs=placed,
        out_specs=(
            P("fsdp", None, "dp"),
            P("fsdp", None, "dp"),
            P("fsdp", None, "dp"),
            P("fsdp", None, "dp"),
        ),
        check_vma=False,
    )
```

```python
import functools

import jax
import jax.numpy as jnp
from jax import lax
from jax.experimental import pallas as pl
from jax.experimental.pallas import tpu as pltpu
from jax.sharding import PartitionSpec as P

STEP = 8


beta_first = 0.9
beta_second = 0.95
learn_rate = 0.001
weight_decay = 0.1
epsilon = 1e-08


def adam_update(gradient, moment_one, moment_two, weights):
    moment_one_new = beta_first * moment_one + (1.0 - beta_first) * gradient
    moment_two_new = beta_second * moment_two + (1.0 - beta_second) * gradient * gradient
    correct_one = 1.0 - beta_first**STEP
    correct_two = 1.0 - beta_second**STEP
    update = (
        moment_one_new / correct_one / (jnp.sqrt(moment_two_new / correct_two) + epsilon)
        + weight_decay * weights
    )
    return (moment_one_new, moment_two_new, weights - learn_rate * update)


def shards(inputs, value_cotangent, master, first_moment, second_moment):
    _, heads, slice_width = master.shape
    head_size = value_cotangent.shape[1] // heads
    head_parts = []
    for head in range(heads):
        head_cot = value_cotangent[:, head * head_size : (head + 1) * head_size]
        head_term = lax.dot_general(
            inputs, head_cot, (((0,), (0,)), ((), ())), preferred_element_type=jnp.float32
        )
        head_parts.append(
            lax.psum_scatter(
                head_term.astype(jnp.bfloat16), "dp", scatter_dimension=1, tiled=True
            ).astype(jnp.float32)
        )
    column_part = jnp.stack(head_parts, axis=1)
    grad_share = lax.psum_scatter(column_part, "fsdp", scatter_dimension=0, tiled=True)
    moment_one_new, moment_two_new, master_new = adam_update(
        grad_share, first_moment, second_moment, master
    )
    narrow_weight = master_new.astype(jnp.bfloat16)
    gathered = lax.all_gather(narrow_weight, "fsdp", axis=0, tiled=True)
    head_index = lax.axis_index("fsdp") % heads
    picked = lax.dynamic_slice_in_dim(gathered, head_index, 1, 1)
    tp_block = picked.reshape(1, gathered.shape[0], slice_width)
    return (moment_one_new, moment_two_new, master_new, tp_block)


VMEM_BYTES = 67043328
SPARE_BYTES = 64 * 1024
PLANE = 8


def step_kernel(
    n, pieces, x_hbm, g_hbm, w_hbm, m_hbm, v_hbm, m_out, v_out, w_out, tp_out,
    x_ref, g_ref, w_ref, m_ref, v_ref,
    total, mate_part, mate_in, parts, first_in, relay, second_in,
    column_part, column_in, line_in, line_sum, plane_part, plane_in, blocks,
    load_sem, mate_send, mate_recv, plane_send, first_recv, second_recv,
    column_send, column_recv, row_send, row_recv, far_send, side_send, side_recv,
    line_recv, plane_recv, up_sem, down_sem,
):
    me = lax.axis_index("fsdp")
    z = me // PLANE
    q = lax.rem(me, PLANE)
    y = q // 4
    x = lax.rem(q // 2, 2)
    core = lax.rem(q, 2)
    mate = me + 1 - 2 * core
    x_mate = me + 2 - 4 * x
    y_mate = me + 4 - 8 * y
    xy_mate = x_mate + 4 - 8 * y
    depth = n // PLANE
    layers = depth // 2
    rows, heads, head_size = w_ref.shape
    half = x_ref.shape[1] // 2
    tile = half // layers
    worker = z // layers

    def mirrored(place):
        return place + worker * (depth - 1 - 2 * place)

    inward = mirrored(z)

    def layer(side, t):
        return t + side * (depth - 1 - 2 * t)

    def columns(side, t):
        return pl.ds(pl.multiple_of(layer(side, t) * tile, 128), tile)

    tiles = [(side, t) for side in (1 - core, core) for t in range(layers)]
    load_g = pltpu.make_async_copy(g_hbm, g_ref, load_sem.at[0])
    load_x = [
        pltpu.make_async_copy(
            x_hbm.at[:, columns(*place)], x_ref.at[:, columns(*place)], load_sem.at[2 + i]
        )
        for i, place in enumerate(tiles)
    ]
    load_state = [
        pltpu.make_async_copy(source, target, load_sem.at[1])
        for source, target in ((w_hbm, w_ref), (m_hbm, m_ref), (v_hbm, v_ref))
    ]
    load_g.start()
    for load in load_x + load_state:
        load.start()

    def to(device):
        return dict(device_id={"fsdp": device}, device_id_type=pl.DeviceIdType.MESH)

    barrier = pltpu.get_barrier_semaphore()
    for slot in range(4):
        @pl.when(lax.rem(q, 4) != slot)
        def _():
            pl.semaphore_signal(barrier, inc=1, **to(z * PLANE + y * 4 + slot))
    pl.semaphore_signal(barrier, inc=1, **to(y_mate))
    has_lower, has_upper = z > 0, z < depth - 1

    @pl.when(has_lower)
    def _():
        pl.semaphore_signal(barrier, inc=1, **to(me - PLANE))

    @pl.when(has_upper)
    def _():
        pl.semaphore_signal(barrier, inc=1, **to(me + PLANE))

    def point(p):
        for rank, behind, ahead, semaphore, step in (
            (z, has_lower, has_upper, up_sem, PLANE),
            (depth - 1 - z, has_upper, has_lower, down_sem, -PLANE),
        ):
            @pl.when(rank == p if p < POINTS else rank >= p)
            def _():
                @pl.when(behind)
                def _():
                    pl.semaphore_wait(semaphore, 1)

                @pl.when(ahead)
                def _():
                    pl.semaphore_signal(semaphore, inc=1, **to(me + step))

    def dot_tile(side, t):
        return lax.dot_general(
            x_ref[:, columns(side, t)], g_ref[...], (((0,), (0,)), ((), ())),
            preferred_element_type=jnp.float32,
        ).reshape(2, 2, 2, rows, heads * head_size)

    def span_of(k):
        start, count = pieces[k][:2]
        return pl.ds(start, count)

    def slice_of(k):
        start, count = pieces[k][:2]
        return slice(start, start + count)

    def mate_copy(k, t):
        span = span_of(k)
        return pltpu.make_async_remote_copy(
            mate_part.at[t, :, :, :, span], mate_in.at[t, :, :, :, span],
            mate_send, mate_recv.at[k * layers + t], **to(mate)
        )

    def first_copies(k, t):
        span = span_of(k)
        arrived = first_recv.at[k * layers + t]
        if t % 2 == 0:
            moves = ((parts.at[t, :, 1 - x, :, span], first_in.at[t, :, :, span], x_mate),)
        else:
            moves = ((parts.at[t, 1 - y, :, :, span], first_in.at[t, :, :, span], y_mate),)
        return [
            pltpu.make_async_remote_copy(source, target, plane_send, arrived, **to(device))
            for source, target, device in moves
        ]

    def second_copy(k, t):
        span = span_of(k)
        return pltpu.make_async_remote_copy(
            relay.at[t, :, span], second_in.at[t, :, span],
            plane_send, second_recv.at[k * layers + t],
            **to(y_mate if t % 2 == 0 else x_mate)
        )

    def column_copy(k, t, side):
        span = span_of(k)
        return pltpu.make_async_remote_copy(
            column_part.at[t, side, span], column_in.at[z, span],
            column_send, column_recv.at[k],
            **to(layer(core, t) * PLANE + 2 * (q // 2) + side),
        )

    def drain(block, semaphore):
        pltpu.make_async_copy(block, block, semaphore).wait()

    def join(k, t):
        span = slice_of(k)
        with jax.named_scope(f"mate{k}_{t}"):
            mate_copy(k, t).wait_recv()
        value = (
            total[t, :, :, :, span] + mate_in[t, :, :, :, span].astype(jnp.float32)
        ).astype(jnp.bfloat16)
        parts[t, :, :, :, span] = value
        if pieces[k][2]:
            for copy in first_copies(k, t):
                copy.start()
            return
        for side in range(2):
            own = jnp.logical_and(layer(core, t) == z, core == side)

            @pl.when(jnp.logical_not(own))
            def _():
                pltpu.make_async_remote_copy(
                    parts.at[t, :, :, side, span_of(k)], line_in.at[z], plane_send, line_recv,
                    **to(layer(core, t) * PLANE + 2 * (q // 2) + side)
                ).start()

            @pl.when(own)
            def _():
                line_in[z] = value[:, :, side]

    def across(k):
        with jax.named_scope(f"line{k}"):
            for sources, here in ((depth - 1, worker == core), (depth, worker != core)):
                @pl.when(here)
                def _():
                    drain(line_in.at[pl.ds(0, sources)], line_recv)
        value = line_in[0].astype(jnp.float32)
        for source in range(1, depth):
            value = value + line_in[source].astype(jnp.float32)
        plane_part[...] = value.astype(jnp.bfloat16)
        for slot, (row, column_at, device) in enumerate(
            ((y, 1 - x, x_mate), (1 - y, x, y_mate), (1 - y, 1 - x, xy_mate))
        ):
            pltpu.make_async_remote_copy(
                plane_part.at[row, column_at], plane_in.at[slot], plane_send, plane_recv,
                **to(device)
            ).start()
        own = line_in[0, y, x].astype(jnp.float32)
        for source in range(1, depth):
            own = own + line_in[source, y, x].astype(jnp.float32)
        line_sum[...] = own

    def second(k):
        span = slice_of(k)
        for t in range(layers):
            with jax.named_scope(f"first{k}_{t}"):
                drain(first_in.at[t, :, :, span_of(k)], first_recv.at[k * layers + t])
            if t % 2 == 0:
                own, came = parts[t, 1 - y, x, :, span], first_in[t, 1 - y, :, span]
            else:
                own, came = parts[t, y, 1 - x, :, span], first_in[t, 1 - x, :, span]
            relay[t, :, span] = (
                own.astype(jnp.float32) + came.astype(jnp.float32)
            ).astype(jnp.bfloat16)
            second_copy(k, t).start()

    def column(k):
        span = slice_of(k)
        for t in range(layers):
            with jax.named_scope(f"second{k}_{t}"):
                second_copy(k, t).wait_recv()
            came = first_in[t, y if t % 2 == 0 else x, :, span].astype(jnp.float32)
            value = (
                parts[t, y, x, :, span].astype(jnp.float32)
                + came
                + second_in[t, :, span].astype(jnp.float32)
            ).astype(jnp.bfloat16)
            column_part[t, :, span] = value
            for side in range(2):
                own = jnp.logical_and(layer(core, t) == z, core == side)

                @pl.when(jnp.logical_not(own))
                def _():
                    column_copy(k, t, side).start()

                @pl.when(own)
                def _():
                    column_in[z, span] = value[side]

    def target_of(layer_to, head):
        return layer_to * PLANE + y * 4 + head

    def reach(k):
        return layers + 1 if pieces[k][3] else depth

    def row_copy(k, layer_to, head):
        span = span_of(k)
        return pltpu.make_async_remote_copy(
            blocks.at[head, span], tp_out.at[me, span],
            row_send, row_recv.at[k * depth + z], **to(target_of(layer_to, head))
        )

    def update(k):
        span = slice_of(k)
        with jax.named_scope(f"column{k}"):
            if pieces[k][2]:
                for sources, here in ((depth - 1, worker == core), (depth, worker != core)):
                    @pl.when(here)
                    def _():
                        drain(column_in.at[pl.ds(0, sources), span_of(k)], column_recv.at[k])
                gradients = column_in[0, span].astype(jnp.float32)
                for source in range(1, depth):
                    gradients = gradients + column_in[source, span].astype(jnp.float32)
            else:
                drain(plane_in, plane_recv)
                gradients = line_sum[...]
                for source in range(3):
                    gradients = gradients + plane_in[source].astype(jnp.float32)
        news = []
        for head in range(heads):
            m_new, v_new, w_new = adam_update(
                gradients[:, head * head_size : (head + 1) * head_size],
                m_ref[span, head, :], v_ref[span, head, :], w_ref[span, head, :],
            )
            narrow = w_new.astype(jnp.bfloat16)
            blocks[head, span] = narrow
            news.append((m_new, v_new, w_new))
        for place in reversed(range(reach(k))):
            for head in range(heads):
                target = target_of(mirrored(place), head)

                @pl.when(target != me)
                def _():
                    row_copy(k, mirrored(place), head).start()

        for head in range(heads):
            pltpu.make_async_remote_copy(
                blocks.at[head, span_of(k)], tp_out.at[me, span_of(k)], row_send, side_recv,
                **to(z * PLANE + (1 - y) * 4 + head)
            ).start()
        tp_out[me, span] = blocks[lax.rem(q, 4), span]
        for head, (m_new, v_new, w_new) in enumerate(news):
            m_out[span, head, :] = m_new
            v_out[span, head, :] = v_new
            w_out[span, head, :] = w_new

    def group_copy(k, layer_from, device, send, recv):
        block = tp_out.at[pl.ds(layer_from * PLANE + y * 4, 4), span_of(k)]
        return pltpu.make_async_remote_copy(block, block, send, recv, **to(device))

    def forward(k, places, relayed, crossed):
        for place in places:
            layer_from = mirrored(place)
            arrived = row_recv.at[k * depth + layer_from]
            with jax.named_scope(f"row{k}_{place}"):
                if place < layers:
                    for slabs, here in ((3, inward == place), (4, inward != place)):
                        @pl.when(here)
                        def _():
                            drain(tp_out.at[pl.ds(0, slabs), span_of(k)], arrived)
                else:
                    drain(tp_out.at[pl.ds(0, 4), span_of(k)], arrived)
            for other in range(layers - 1 if relayed else 0):
                there = mirrored(other) * PLANE + q
                group_copy(k, layer_from, there, far_send, arrived).start()
                if relayed == 2:
                    group_copy(k, layer_from, there + y_mate - me, far_send, side_recv).start()
            if not crossed:
                continue
            if place >= layers:
                group_copy(k, layer_from, y_mate, side_send, side_recv).start()
            else:
                @pl.when(inward != place)
                def _():
                    group_copy(k, layer_from, y_mate, side_send, side_recv).start()

    def near(k):
        forward(k, range(layers), 0, True)

    def gate(k):
        @pl.when(inward == layers - 1)
        def _():
            forward(k, range(layers, depth), pieces[k][3], True)

    def end(k):
        @pl.when(inward != layers - 1)
        def _():
            forward(k, range(layers, depth), 0, pieces[k][3] != 2)

    with jax.named_scope("loads"):
        load_g.wait()
    for t in range(layers):
        with jax.named_scope(f"load{t}"):
            load_x[t].wait()
        mate_part[t] = dot_tile(1 - core, t).astype(jnp.bfloat16)
        if t == 0:
            with jax.named_scope("barrier"):
                pl.semaphore_wait(
                    barrier, 4 + has_lower.astype(jnp.int32) + has_upper.astype(jnp.int32)
                )
            point(0)
        mate_copy(0, t).start()
    for k in (1, len(pieces) - 1, *range(2, len(pieces) - 1)):
        for t in range(layers):
            mate_copy(k, t).start()
    for t in range(layers):
        load_x[layers + t].wait()
        total[t] = dot_tile(core, t)
    for load in load_state:
        load.wait()
    for action, k in ORDER:
        if action == "join":
            for t in range(layers):
                join(k, t)
        elif action == "point":
            with jax.named_scope(f"point{k}"):
                point(k)
        elif action == "second":
            second(k)
        elif action == "column":
            column(k)
        elif action == "across":
            across(k)
        elif action == "update":
            update(k)
        else:
            {"near": near, "gate": gate, "end": end}[action](k)

    with jax.named_scope("sends"):
        drain(mate_part, mate_send)
        for k in range(len(pieces)):
            span = span_of(k)
            if pieces[k][2]:
                drain(first_in.at[:, :, :, span], plane_send)
                drain(relay.at[:, :, span], plane_send)
            else:
                drain(plane_in, plane_send)
                for _ in range(layers * 2 - 1):
                    drain(plane_part, plane_send)

                @pl.when(worker != core)
                def _():
                    drain(plane_part, plane_send)
        for k in range(len(pieces)):
            if not pieces[k][2]:
                continue
            for sides, here in ((1, worker == core), (2, worker != core)):
                @pl.when(here)
                def _():
                    for t in range(layers):
                        drain(
                            column_part.at[t, pl.ds(0, sides if t == 0 else 2), span_of(k)],
                            column_send,
                        )
        for k in range(len(pieces)):
            drain(tp_out.at[pl.ds(0, heads * (reach(k) + 1) - 1), span_of(k)], row_send)
            if pieces[k][3] and layers > 1:
                @pl.when(inward == layers - 1)
                def _():
                    for _ in range((layers - 1) * pieces[k][3]):
                        drain(tp_out.at[pl.ds(0, 4 * layers), span_of(k)], far_send)
            for slabs, here in (
                ((depth - 1) * 4, inward == layers - 1),
                (((layers if pieces[k][3] == 2 else depth) - 1) * 4, inward != layers - 1),
            ):
                @pl.when(here)
                def _():
                    drain(tp_out.at[pl.ds(0, slabs), span_of(k)], side_send)
        slabs = tp_out.at[pl.ds(0, depth * 4)]
    with jax.named_scope("last"):
        drain(slabs, side_recv)


POINTS = 3
PARTS = ((16, True, 1), (16, True, 1), (16, True, 1), (16, True, 2), (16, False, 1))
ORDER = (
    ("join", 0), ("join", 1), ("join", 2), ("point", 1), ("point", 2), ("point", 3),
    ("join", 4), ("second", 0), ("join", 3), ("second", 1), ("second", 2), ("column", 0),
    ("second", 3), ("column", 1), ("across", 4), ("column", 2), ("update", 0), ("column", 3),
    ("update", 1), ("near", 0), ("update", 4), ("gate", 0), ("update", 2), ("near", 1),
    ("update", 3), ("gate", 1), ("near", 4), ("gate", 4), ("end", 0), ("near", 2), ("gate", 2),
    ("near", 3), ("gate", 3), ("end", 1), ("end", 4), ("end", 2), ("end", 3),
)


def row_pieces(rows):
    pieces, start = [], 0
    for i, (share, twice, deputed) in enumerate(PARTS):
        count = rows - start if i + 1 == len(PARTS) else share
        pieces.append((start, count, twice, deputed))
        start += count
    return tuple(pieces)


def finish_kernel(*refs):
    count = (len(refs) - 1) // 2
    copies = [
        pltpu.make_async_copy(refs[i], refs[count + i], refs[-1].at[i])
        for i in range(count)
    ]
    for copy in copies:
        copy.start()
    for copy in copies:
        copy.wait()


def fused(n, inputs, value_cotangent, master, first_moment, second_moment):
    tokens, features = inputs.shape
    width = value_cotangent.shape[1]
    rows, heads, head_size = master.shape
    depth = n // PLANE
    layers = depth // 2
    pieces = row_pieces(rows)
    state = jax.ShapeDtypeStruct(master.shape, jnp.float32)
    slabs = jax.ShapeDtypeStruct((n, rows, head_size), jnp.bfloat16)
    block = jax.ShapeDtypeStruct((1, features, head_size), jnp.bfloat16)
    results = 12 * master.size + 2 * block.size + SPARE_BYTES
    vmem = pl.BlockSpec(memory_space=pltpu.VMEM)
    narrow = jnp.bfloat16
    dma = pltpu.SemaphoreType.DMA
    held = pl.pallas_call(
        functools.partial(step_kernel, n, pieces),
        out_shape=tuple(pltpu.VMEM(a.shape, a.dtype) for a in (state, state, state, slabs)),
        in_specs=[pl.BlockSpec(memory_space=pltpu.HBM)] * 5,
        out_specs=[vmem] * 4,
        scratch_shapes=[
            pltpu.VMEM((tokens, features), narrow),
            pltpu.VMEM((tokens, width), narrow),
            pltpu.VMEM(master.shape, jnp.float32),
            pltpu.VMEM(master.shape, jnp.float32),
            pltpu.VMEM(master.shape, jnp.float32),
            pltpu.VMEM((layers, 2, 2, 2, rows, width), jnp.float32),
            pltpu.VMEM((layers, 2, 2, 2, rows, width), narrow),
            pltpu.VMEM((layers, 2, 2, 2, rows, width), narrow),
            pltpu.VMEM((layers, 2, 2, 2, rows, width), narrow),
            pltpu.VMEM((layers, 2, 2, rows, width), narrow),
            pltpu.VMEM((layers, 2, rows, width), narrow),
            pltpu.VMEM((layers, 2, rows, width), narrow),
            pltpu.VMEM((layers, 2, rows, width), narrow),
            pltpu.VMEM((depth, rows, width), narrow),
            pltpu.VMEM((depth, 2, 2, pieces[-1][1], width), narrow),
            pltpu.VMEM((pieces[-1][1], width), jnp.float32),
            pltpu.VMEM((2, 2, pieces[-1][1], width), narrow),
            pltpu.VMEM((3, pieces[-1][1], width), narrow),
            pltpu.VMEM((heads, rows, head_size), narrow),
            dma((2 + 2 * layers,)),
            dma,
            dma((layers * len(pieces),)),
            dma,
            dma((layers * (len(pieces) - 1),)),
            dma((layers * (len(pieces) - 1),)),
            dma,
            dma((len(pieces) - 1,)),
            dma,
            dma((depth * len(pieces),)),
            dma,
            dma,
            dma,
            dma,
            dma,
            pltpu.SemaphoreType.REGULAR,
            pltpu.SemaphoreType.REGULAR,
        ],
        compiler_params=pltpu.CompilerParams(
            collective_id=0, has_side_effects=True, vmem_limit_bytes=VMEM_BYTES - results
        ),
    )(inputs, value_cotangent, master, first_moment, second_moment)
    held = held[:3] + (held[3].reshape(block.shape),)
    return pl.pallas_call(
        finish_kernel,
        out_shape=(state, state, state, block),
        in_specs=[vmem] * 4,
        out_specs=[pl.BlockSpec(memory_space=pltpu.HBM)] * 4,
        scratch_shapes=[dma((4,))],
        compiler_params=pltpu.CompilerParams(vmem_limit_bytes=VMEM_BYTES // 2),
    )(*held)


def solution(mesh):
    n = mesh.shape["fsdp"]

    def body(inputs, value_cotangent, master, first_moment, second_moment):
        rows = master.shape[0]
        direct = (
            mesh.shape["dp"] == 1
            and n % (2 * PLANE) == 0
            and inputs.shape[1] % (256 * (n // (2 * PLANE))) == 0
            and rows % 16 == 0
            and rows > sum(part[0] for part in PARTS[:-1])
            and master.shape[1] * 2 == PLANE
            and master.shape[2] % 128 == 0
        )
        if direct:
            return fused(n, inputs, value_cotangent, master, first_moment, second_moment)
        return shards(inputs, value_cotangent, master, first_moment, second_moment)

    placed = (
        P(("fsdp", "dp"), None),
        P(("fsdp", "dp"), None),
        P("fsdp", None, "dp"),
        P("fsdp", None, "dp"),
        P("fsdp", None, "dp"),
    )
    return jax.shard_map(
        body,
        mesh=mesh,
        in_specs=placed,
        out_specs=(
            P("fsdp", None, "dp"),
            P("fsdp", None, "dp"),
            P("fsdp", None, "dp"),
            P("fsdp", None, "dp"),
        ),
        check_vma=False,
    )
```
